128 devices in a mesh: rows: 16 (over z_hi, x, core), cols: 8 (over z_lo, y).
Axes of the slice: x: 4, y: 4, z: 4 (z_hi: 2, z_lo: 2; z = z_hi * 2 + z_lo), core: 2. Of those that a mesh axis runs over, the one named last changes fastest.
Arguments:
- surface_field: float32 [8192, 16384], P('rows', 'cols'), may hold values from -20 to 30
- land_words: int32 [8192, 512], P('rows', 'cols'), may hold values from -2147483648 to 2147483646
Outputs:
- level_one: float32 [4096, 8192], P('rows', 'cols')
- level_two: float32 [2048, 4096], P('rows', 'cols')
- level_three: float32 [1024, 2048], P('rows', 'cols')
- level_four: float32 [512, 1024], P('rows', 'cols')
- level_means: float32 [4], replicated
- level_maxima: float32 [4], replicated
The draws below stay inside these ranges and needn't reach their ends.
All inputs are finite; a program needn't handle non-finite values.
Results may differ from the reference program's by a relative error of at most 0.0001.
Values sent between devices are 32-bit elements; how exact they have to be, the bound alone decides.
No kernel may reach another device: no remote copies, remote signals or barrier semaphores. Data moves between devices by JAX's collectives and lax.ppermute only.
A program may use at most 128 MiB of HBM per device.

```python
import math
import jax
import jax.numpy as jnp

NY = 8192
NX = 16384


def draw_surface_field(key, part):
    noise_key = jax.random.fold_in(jax.random.fold_in(key, 11), 0)
    rows_frac = jnp.arange(NY, dtype=jnp.float32) / NY
    cols_frac = jnp.arange(NX, dtype=jnp.float32) / NX
    trend = (1.0 + 2.0 * rows_frac)[:, None] * (1.0 + 2.0 * cols_frac)[None, :]
    noise = jnp.clip(jax.random.normal(noise_key, (NY, NX), jnp.float32), -6.0, 6.0)
    return (trend + noise).astype(jnp.float32)


def touch_ends(values, key, smallest, top_value):
    index_at = [jax.random.randint(jax.random.fold_in(key, axis), (), 0, length) for axis, length in enumerate(values.shape)]
    main_axis = values.shape.index(max(values.shape))
    next_to = index_at[:main_axis] + [(index_at[main_axis] + 1) % values.shape[main_axis]] + index_at[main_axis + 1:]
    return values.at[tuple(index_at)].set(smallest).at[tuple(next_to)].set(top_value)


def setup_inputs(seed: int = 0) -> dict:
    splits = jax.random.split(jax.random.key(seed), 3)
    surface_field = draw_surface_field(jax.random.fold_in(splits[2], 71), 0)
    land_words = touch_ends(jax.random.randint(splits[1], (NY, NX // 32), -2147483648, 2147483647), jax.random.fold_in(splits[1], 1), -2147483648, 2147483646).astype(jnp.int32)
    return dict(surface_field=surface_field, land_words=land_words)


stencil_weights = (0.125, 0.375, 0.375, 0.125)
floor_value = 0.05
mean_eps = 1e-6


def coarsen(extended):
    count_rows = (extended.shape[1] - 2) // 2
    count_cols = (extended.shape[2] - 2) // 2
    across = stencil_weights[0] * extended[:, :, 0:2 * count_cols:2]
    for offset in range(1, 4):
        across = across + stencil_weights[offset] * extended[:, :, offset:offset + 2 * count_cols:2]
    downward = stencil_weights[0] * across[:, 0:2 * count_rows:2, :]
    for offset in range(1, 4):
        downward = downward + stencil_weights[offset] * across[:, offset:offset + 2 * count_rows:2, :]
    return downward


def finish(partial_value):
    values = partial_value[0] / jnp.maximum(partial_value[1], floor_value)
    covers = partial_value[1]
    return values, covers, jnp.stack([covers * values, covers])


def reference(surface_field, land_words):
    expanded = jnp.repeat(land_words, 32, axis=1)
    shifts = jnp.arange(expanded.shape[1], dtype=jnp.int32) % 32
    land_flag = jnp.bitwise_and(jnp.right_shift(expanded, shifts[None, :]), 1)
    rows_index = jnp.arange(NY, dtype=jnp.int32).astype(jnp.float32)
    latitude = ((rows_index + 0.5) / NY - 0.5) * math.pi
    covers = land_flag.astype(jnp.float32) * jnp.cos(latitude)[:, None]
    stacked = jnp.stack([covers * surface_field, covers])
    outputs = []
    weighted = []
    totals = []
    maxima = []
    for level_step in range(4):
        wrapped = jnp.concatenate([stacked[:, :, -1:], stacked, stacked[:, :, :1]], axis=2)
        padded = jnp.pad(wrapped, ((0, 0), (1, 1), (0, 0)))
        values, covers, stacked = finish(coarsen(padded))
        outputs.append(values)
        weighted.append(jnp.sum(stacked[0]))
        totals.append(jnp.sum(covers))
        maxima.append(jnp.max(values))
    level_means = jnp.stack(weighted) / (jnp.stack(totals) + mean_eps)
    return outputs[0], outputs[1], outputs[2], outputs[3], level_means, jnp.stack(maxima)
```

```python
import math

import jax
import jax.numpy as jnp
import numpy as np
from jax import lax
from jax.experimental import pallas as pl
from jax.experimental.pallas import tpu as pltpu
from jax.sharding import Mesh
from jax.sharding import PartitionSpec as P

ROWS = ("rows_0", "rows_1", "rows_2")
COLS = ("cols_0", "cols_1")
CHIPS = ("rows_0", "rows_1", "cols_0", "cols_1")
CORE = "rows_2"


stencil_weights = (0.125, 0.375, 0.375, 0.125)
floor_value = 0.05
mean_eps = 1e-06

f32 = jnp.float32
bf16 = jnp.bfloat16


def band_main():
    table = np.zeros((256, 256), np.float32)
    for j in range(128):
        for a in range(4):
            k = 2 * j - 1 + a
            if 0 <= k < 256:
                table[k, j] = stencil_weights[a]
    table[255, 128] = stencil_weights[0]
    table[0, 255] = stencil_weights[3]
    return table


def band_halo(width, right, left):
    table = np.zeros((128, 256), np.float32)
    for j in range(width // 2):
        for a in range(4):
            k = 2 * j - 1 + a
            if 0 <= k < width:
                table[right + k, j] = stencil_weights[a]
        for a in range(4):
            k = -3 - 2 * j + a
            if -width <= k < 0:
                table[left + k, 127 - j] = stencil_weights[a]
    table[left - 1, 128] = stencil_weights[0]
    table[right, 255] = stencil_weights[3]
    return table


def lane_iota(shape):
    return lax.broadcasted_iota(jnp.int32, shape, 1)


def words_wide(words):
    return jnp.concatenate([words, words], axis=1)


def land_mask(wide, tile):
    lane = lane_iota(wide.shape)
    place = 4 * tile + lax.shift_right_logical(lane, 5)
    word = jnp.take_along_axis(wide, place, axis=1, mode="promise_in_bounds")
    return (word & lax.shift_left(jnp.int32(1), lane & 31)) != 0


def split(x):
    high = x.astype(bf16)
    low = (x - high.astype(f32)).astype(bf16)
    return high, low


def dot(a, b):
    return jnp.dot(a, b, preferred_element_type=f32)


def rows_down(ref, start, count, *rest):
    index = lambda a: (*rest, pl.ds(start + a, count, stride=2), slice(None))
    outer = ref[index(0)] + ref[index(3)]
    inner = ref[index(1)] + ref[index(2)]
    return stencil_weights[0] * outer + stencil_weights[1] * inner


def columns_kernel(left_ref, right_ref, words_ref, to_left_ref, to_right_ref):
    wide = words_wide(words_ref[...])
    left_mask = land_mask(wide, 0)
    right_mask = land_mask(wide, 15)
    lane = lane_iota(left_mask.shape)
    left_land = pltpu.roll(jnp.where(left_mask, 1.0, 0.0), 16, 1)
    right_land = pltpu.roll(jnp.where(right_mask, 1.0, 0.0), 112, 1)
    left_side = jnp.where(lane < 16, jnp.where(left_mask, left_ref[...], 0.0), left_land)
    right_side = jnp.where(lane >= 112, jnp.where(right_mask, right_ref[...], 0.0), right_land)
    both = jnp.where(lane < 64, left_side, right_side).T
    to_left_ref[...] = both[0:32]
    to_right_ref[...] = both[96:128]


def columns_strips(field, words):
    rows = field.shape[0]
    return pl.pallas_call(
        columns_kernel,
        grid=(1,),
        in_specs=[
            pl.BlockSpec((rows, 128), lambda i: (0, 0)),
            pl.BlockSpec((rows, 128), lambda i: (0, field.shape[1] // 128 - 1)),
            pl.BlockSpec((rows, 64), lambda i: (0, 0)),
        ],
        out_specs=[pl.BlockSpec((32, rows), lambda i: (0, 0))] * 2,
        out_shape=[jax.ShapeDtypeStruct((32, rows), f32)] * 2,
        name="columns_strips",
    )(field, field, words)


def rows_kernel(
    top_ref, bottom_ref, top_words_ref, bottom_words_ref, right_ref, left_ref,
    up_ref, down_ref, halo_ref,
):
    rows = halo_ref.shape[0]
    for part in range(rows // 128):
        cols = slice(part * 128, part * 128 + 128)
        halo_ref[cols, :] = jnp.concatenate(
            [right_ref[:, cols], jnp.zeros((64, 128), f32), left_ref[:, cols]], axis=0
        ).T
    for field_ref, words_ref, out_ref, first in (
        (top_ref, top_words_ref, up_ref, 0),
        (bottom_ref, bottom_words_ref, down_ref, rows - 16),
    ):
        wide = words_wide(words_ref[...])
        for tile in range(16):
            lanes = slice(tile * 128, tile * 128 + 128)
            mask = land_mask(wide, tile)
            out_ref[0:16, lanes] = jnp.where(mask, field_ref[:, lanes], 0.0)
            out_ref[16:32, lanes] = jnp.where(mask, 1.0, 0.0)
        out_ref[0:16, 2048:2176] = halo_ref[first : first + 16, :]
        out_ref[16:32, 2048:2176] = jnp.zeros((16, 128), f32)


def rows_strips(field, words, from_right, from_left):
    rows, cols = field.shape
    last = rows // 16 - 1
    return pl.pallas_call(
        rows_kernel,
        grid=(1,),
        in_specs=[
            pl.BlockSpec((16, cols), lambda i: (0, 0)),
            pl.BlockSpec((16, cols), lambda i: (last, 0)),
            pl.BlockSpec((16, 64), lambda i: (0, 0)),
            pl.BlockSpec((16, 64), lambda i: (last, 0)),
            pl.BlockSpec((32, rows), lambda i: (0, 0)),
            pl.BlockSpec((32, rows), lambda i: (0, 0)),
        ],
        out_specs=[
            pl.BlockSpec((32, cols + 128), lambda i: (0, 0)),
            pl.BlockSpec((32, cols + 128), lambda i: (0, 0)),
            pl.BlockSpec((rows, 128), lambda i: (0, 0)),
        ],
        out_shape=[
            jax.ShapeDtypeStruct((32, cols + 128), f32),
            jax.ShapeDtypeStruct((32, cols + 128), f32),
            jax.ShapeDtypeStruct((rows, 128), f32),
        ],
        name="rows_strips",
    )(field, field, words, words, from_right, from_left)


def own_kernel(
    field_ref, words_ref, cos_ref, band_ref, num_ref, den_ref,
    lhs_ref, main_ref, edge_ref, wide_ref, sheet_ref,
):
    step = pl.program_id(0)
    rows = field_ref.shape[0]

    @pl.when(step == 0)
    def _():
        wide_ref[...] = words_wide(words_ref[...])
        zeros = jnp.zeros((2, rows, 128), f32)
        edge_ref[0] = zeros
        edge_ref[9] = zeros
        main_ref[8] = zeros
        sheet_ref[...] = jnp.zeros(sheet_ref.shape, f32)

    @pl.when(step < 8)
    def _():
        chunk = 64
        for half in range(2):
            lanes = slice(half * 128, half * 128 + 128)
            for first in range(0, rows, chunk):
                part = slice(first, first + chunk)
                mask = land_mask(wide_ref[part, :], 2 * step + half)
                high, low = split(jnp.where(mask, field_ref[part, lanes], 0.0))
                lhs_ref[0, part, lanes] = high
                lhs_ref[1, part, lanes] = low
                lhs_ref[2, part, lanes] = jnp.where(mask, 1.0, 0.0).astype(bf16)
        band = band_ref[...]
        product = dot(lhs_ref[0], band) + dot(lhs_ref[1], band)
        cover = dot(lhs_ref[2], band)
        main_ref[step, 0] = product[:, 0:128]
        edge_ref[step + 1, 0] = product[:, 128:256]
        main_ref[step, 1] = cover[:, 0:128]
        edge_ref[step + 1, 1] = cover[:, 128:256]

    @pl.when(step > 0)
    def _():
        tile = step - 1
        after = jnp.where(tile < 8, tile + 2, 1)
        cos = cos_ref[16 : 16 + rows, :]
        low_half = lane_iota((rows, 128)) < 64
        for which, out_ref in ((0, num_ref), (1, den_ref)):
            edges = jnp.where(low_half, edge_ref[tile, which], edge_ref[after, which])
            sheet_ref[which, 24 : 24 + rows, :] = (main_ref[tile, which] + edges) * cos
            out_ref[...] = rows_down(sheet_ref, 7, out_ref.shape[0], which)


def own_level(field, words, cosines, band):
    rows, cols = field.shape
    tiles = cols // 256
    out_rows = rows // 2 + 16
    out = jax.ShapeDtypeStruct((out_rows, cols // 2 + 128), f32)
    out_spec = pl.BlockSpec((out_rows, 128), lambda t: (0, jnp.maximum(t - 1, 0)))
    return pl.pallas_call(
        own_kernel,
        grid=(tiles + 2,),
        in_specs=[
            pl.BlockSpec((rows, 256), lambda t: (0, jnp.minimum(t, tiles - 1))),
            pl.BlockSpec((rows, 64), lambda t: (0, 0)),
            pl.BlockSpec((rows + 32, 128), lambda t: (0, 0)),
            pl.BlockSpec((256, 256), lambda t: (0, 0)),
        ],
        out_specs=[out_spec, out_spec],
        out_shape=[out, out],
        scratch_shapes=[
            pltpu.VMEM((3, rows, 256), bf16),
            pltpu.VMEM((9, 2, rows, 128), f32),
            pltpu.VMEM((10, 2, rows, 128), f32),
            pltpu.VMEM((rows, 128), jnp.int32),
            pltpu.VMEM((2, rows + 48, 128), f32),
        ],
        name="own_level",
    )(field, words, cosines, band)


def fold(x):
    return x.reshape(x.shape[0] // 8, 8, 128)


def levels_kernel(
    ends_ref, num_ref, den_ref, halo_ref, top_ref, bottom_ref, cos_ref,
    band_ref, band_halo_ref, band_mixed_ref,
    one_ref, two_ref, three_ref, four_ref, stats_ref,
    p1_ref, c1_ref, p2_ref, c2_ref, p3_ref, c3_ref, tall_ref, strip_ref, value_ref,
):
    rows = halo_ref.shape[0]
    band = band_ref[...]
    low_half = lane_iota((8, 128)) < 64

    def pick(before, after):
        shape = before.shape
        return jnp.where(lane_iota(shape) < 64, before, after)

    mixed = band_mixed_ref[...]
    tall_ref[:, 0:8, :] = jnp.zeros((4, 8, 128), f32)
    tall_ref[:, 8 + rows + 32 :, :] = jnp.zeros((4, 8, 128), f32)
    for first, count, source in (
        (0, 16, top_ref[0:16, 2048:2176]),
        (16, rows, halo_ref[...]),
        (16 + rows, 16, bottom_ref[0:16, 2048:2176]),
    ):
        high, low = split(source)
        across = dot(high, mixed) + dot(low, mixed)
        cos = cos_ref[first : first + count, :]
        for k in range(4):
            tall_ref[k, 8 + first : 8 + first + count, :] = (
                across[:, k * 128 : k * 128 + 128] * cos
            )
    count = rows // 2 + 16
    add_p, edge_p, add_c, edge_c = (rows_down(tall_ref, 7, count, k) for k in range(4))
    last = 7 * 128
    for source_ref, out_ref, add, edge in (
        (num_ref, p1_ref, add_p, edge_p),
        (den_ref, c1_ref, add_c, edge_c),
    ):
        lower = lane_iota(edge.shape) < 64
        out_ref[:, 0:128] = source_ref[:, 0:128] + jnp.where(lower, edge, 0.0)
        out_ref[:, 128:last] = source_ref[:, 128:last]
        out_ref[:, last : last + 128] = source_ref[:, last : last + 128] + jnp.where(
            lower, 0.0, edge
        )
        out_ref[:, 1024:1152] = source_ref[:, 1024:1152] + add

    strip_ref[...] = jnp.zeros(strip_ref.shape, f32)
    cos_top = cos_ref[0:16, :]
    cos_bottom = cos_ref[16 + rows : 32 + rows, :]
    for side, (ref, cos, first) in enumerate(((top_ref, cos_top, 8), (bottom_ref, cos_bottom, 24))):
        lhs = []
        for t in range(8):
            high, low = split(ref[0:16, t * 256 : t * 256 + 256])
            lhs += [high, low, ref[16:32, t * 256 : t * 256 + 256].astype(bf16)]
        out = dot(jnp.concatenate(lhs, axis=0), band)
        for which in range(2):
            parts = []
            for t in range(8):
                base = t * 48
                if which == 0:
                    parts.append(out[base : base + 16] + out[base + 16 : base + 32])
                else:
                    parts.append(out[base + 32 : base + 48])
            zero = jnp.zeros((16, 128), f32)
            for t in range(9):
                main = parts[t][:, 0:128] if t < 8 else zero
                before = parts[t - 1][:, 128:256] if t > 0 else zero
                after = parts[(t + 1) % 9][:, 128:256] if t != 7 else zero
                strip_ref[side, which, t, first : first + 16, :] = (main + pick(before, after)) * cos
        where = slice(0, 16) if side == 0 else slice(rows // 2, rows // 2 + 16)
        for which, out_ref in ((0, p1_ref), (1, c1_ref)):
            for t in range(9):
                lanes = slice(t * 128, t * 128 + 128)
                extra = rows_down(strip_ref, 7, 16, side, which, t)
                out_ref[where, lanes] = out_ref[where, lanes] + extra

    at_first = ends_ref[0]
    at_last = ends_ref[1]
    sums = []

    def finish(num, den, halo, own):
        value = num / jnp.maximum(den, floor_value)
        row = lax.broadcasted_iota(jnp.int32, num.shape, 0)
        inside = (row >= halo * at_first) & (row < own + halo + (1 - at_last) * 4096)
        cover = jnp.where(inside, den, 0.0)
        return value, cover * value, cover

    level_one_sums = None
    for t in range(9):
        lanes = slice(t * 128, t * 128 + 128)
        value, product, cover = finish(p1_ref[:, lanes], c1_ref[:, lanes], 8, rows // 2)
        p1_ref[:, lanes] = product
        c1_ref[:, lanes] = cover
        if t < 8:
            own = slice(8, 8 + rows // 2)
            one_ref[:, lanes] = value[own]
            new = (
                jnp.sum(fold(product[own]), 0),
                jnp.sum(fold(cover[own]), 0),
                jnp.max(fold(value[own]), 0),
            )
            if level_one_sums is None:
                level_one_sums = new
            else:
                old = level_one_sums
                level_one_sums = (
                    old[0] + new[0], old[1] + new[1], jnp.maximum(old[2], new[2])
                )
    sums.append(level_one_sums)

    def next_level(p_ref, c_ref, tiles, in_rows, out_rows, halo, own_rows, out_ref, p_out, c_out):
        total = None
        nums = []
        dens = []
        for ref, dest in ((p_ref, nums), (c_ref, dens)):
            blocks = []
            for t in range(tiles):
                high, low = split(ref[:, t * 256 : t * 256 + 256])
                blocks.append(dot(high, band) + dot(low, band))
            high, low = split(ref[:, tiles * 256 : tiles * 256 + 128])
            ring = band_halo_ref[...]
            blocks.append(dot(high, ring) + dot(low, ring))
            count = tiles + 1
            for t in range(count):
                across = blocks[t][:, 0:128] + pick(
                    blocks[(t - 1) % count][:, 128:256], blocks[(t + 1) % count][:, 128:256]
                )
                slot = t % 4
                tall_ref[slot, 8 : 8 + in_rows, :] = across
                tall_ref[slot, 8 + in_rows : 2 * out_rows + 16, :] = jnp.zeros(
                    (2 * out_rows + 8 - in_rows, 128), f32
                )
                dest.append(rows_down(tall_ref, 7, out_rows, slot))
        for t in range(tiles + 1):
            value, product, cover = finish(nums[t], dens[t], halo, own_rows)
            if p_out is not None:
                p_out[:, t * 128 : t * 128 + 128] = product
                c_out[:, t * 128 : t * 128 + 128] = cover
            if t < tiles:
                own = slice(halo, halo + own_rows)
                value_ref[0, 0:out_rows, :] = value
                value_ref[1, 0:out_rows, :] = product
                value_ref[2, 0:out_rows, :] = cover
                v, p, c = (value_ref[k, own, :] for k in range(3))
                out_ref[:, t * 128 : t * 128 + 128] = v
                new = (jnp.sum(fold(p), 0), jnp.sum(fold(c), 0), jnp.max(fold(v), 0))
                total = (
                    new
                    if total is None
                    else (total[0] + new[0], total[1] + new[1], jnp.maximum(total[2], new[2]))
                )
        sums.append(total)

    next_level(p1_ref, c1_ref, 4, 272, 136, 4, 128, two_ref, p2_ref, c2_ref)
    next_level(p2_ref, c2_ref, 2, 136, 72, 2, 64, three_ref, p3_ref, c3_ref)
    next_level(p3_ref, c3_ref, 1, 72, 40, 1, 32, four_ref, None, None)

    lane = lane_iota((1, 128))
    row = jnp.zeros((1, 128), f32)
    for level in range(4):
        for kind in range(3):
            part = sums[level][kind]
            one = (jnp.max if kind == 2 else jnp.sum)(part, axis=0, keepdims=True)
            one = (jnp.max if kind == 2 else jnp.sum)(one, axis=1, keepdims=True)
            row = jnp.where(lane == kind * 4 + level, one, row)
    stats_ref[...] = row


def all_levels(ends, num, den, halo, top, bottom, cosines, band, ring, mixed, rows, cols):
    vmem = pl.BlockSpec(memory_space=pltpu.VMEM)
    outs = [jax.ShapeDtypeStruct((rows >> k, cols >> k), f32) for k in (1, 2, 3, 4)]
    half = rows // 2 + 16
    return pl.pallas_call(
        levels_kernel,
        in_specs=[pl.BlockSpec(memory_space=pltpu.SMEM)] + [vmem] * 9,
        out_specs=[vmem] * 5,
        out_shape=outs + [jax.ShapeDtypeStruct((1, 128), f32)],
        scratch_shapes=[
            pltpu.VMEM((half, cols // 2 + 128), f32),
            pltpu.VMEM((half, cols // 2 + 128), f32),
            pltpu.VMEM((136, cols // 4 + 128), f32),
            pltpu.VMEM((136, cols // 4 + 128), f32),
            pltpu.VMEM((72, cols // 8 + 128), f32),
            pltpu.VMEM((72, cols // 8 + 128), f32),
            pltpu.VMEM((4, rows + 48, 128), f32),
            pltpu.VMEM((2, 2, 9, 48, 128), f32),
            pltpu.VMEM((3, 136, 128), f32),
        ],
        name="all_levels",
    )(ends, num, den, halo, top, bottom, cosines, band, ring, mixed)


def per_device(surface_field, land_words):
    rows, cols = surface_field.shape
    row_devices = lax.axis_size(ROWS)
    col_devices = lax.axis_size(COLS)
    total_rows = rows * row_devices
    position = lax.axis_index(ROWS)

    band = jnp.asarray(band_main(), bf16)
    ring = jnp.asarray(band_halo(64, 0, 128), bf16)
    mixed = jnp.asarray(
        np.concatenate([band_halo(16, 0, 128), band_halo(16, 16, 112)], axis=1), bf16
    )

    global_rows = position * rows - 16 + jnp.arange(rows + 32, dtype=jnp.int32)
    latitude = ((global_rows.astype(f32) + 0.5) / total_rows - 0.5) * math.pi
    cosines = jnp.where((global_rows >= 0) & (global_rows < total_rows), jnp.cos(latitude), 0.0)
    cosines = jnp.broadcast_to(cosines[:, None], (rows + 32, 128))
    ends = jnp.stack([position == 0, position == row_devices - 1]).astype(jnp.int32)

    east = [(i, (i + 1) % col_devices) for i in range(col_devices)]
    west = [(target, source) for source, target in east]
    south = [(i, i + 1) for i in range(row_devices - 1)]
    north = [(target, source) for source, target in south]

    to_left, to_right = columns_strips(surface_field, land_words)
    from_right = lax.ppermute(to_left, COLS, west)
    from_left = lax.ppermute(to_right, COLS, east)
    num, den = own_level(surface_field, land_words, cosines, band)
    to_up, to_down, halo = rows_strips(surface_field, land_words, from_right, from_left)
    bottom = lax.ppermute(to_up, ROWS, north)
    top = lax.ppermute(to_down, ROWS, south)
    one, two, three, four, stats = all_levels(
        ends, num, den, halo, top, bottom, cosines, band, ring, mixed, rows, cols
    )

    is_sum = jnp.arange(128) < 8
    other = lax.ppermute(stats, CORE, [(0, 1), (1, 0)])
    stats = jnp.where(is_sum, stats + other, jnp.maximum(stats, other))
    chips = lax.axis_size(CHIPS)
    every = lax.all_to_all(jnp.broadcast_to(stats, (chips, 128)), CHIPS, 0, 0, tiled=True)
    sums = jnp.sum(every[:, 0:8], axis=0)
    maxima = jnp.max(every[:, 8:12], axis=0)
    means = sums[0:4] / (sums[4:8] + mean_eps)
    return (one, two, three, four, means, maxima)


def solution(mesh):
    finer = Mesh(
        mesh.devices.reshape(2, 4, 2, 2, 4), ("rows_0", "rows_1", "rows_2", "cols_0", "cols_1")
    )
    in_specs = (P(ROWS, COLS), P(ROWS, COLS))
    out_specs = (P(ROWS, COLS), P(ROWS, COLS), P(ROWS, COLS), P(ROWS, COLS), P(), P())
    return jax.shard_map(
        per_device, mesh=finer, in_specs=in_specs, out_specs=out_specs, check_vma=False
    )
```

```python
import functools
import math

import jax
import jax.numpy as jnp
import numpy as np
from jax import lax
from jax.experimental import pallas as pl
from jax.experimental.pallas import tpu as pltpu
from jax.sharding import Mesh
from jax.sharding import PartitionSpec as P

ROWS = ("rows_0", "rows_1", "rows_2")
COLS = ("cols_0", "cols_1")
CHIPS = ("rows_0", "rows_1", "cols_0", "cols_1")
CORE = "rows_2"


stencil_weights = (0.125, 0.375, 0.375, 0.125)
floor_value = 0.05
mean_eps = 1e-06

vmem_limit = 20 * 1024 * 1024

f32 = jnp.float32
bf16 = jnp.bfloat16


def band_main():
    table = np.zeros((256, 256), np.float32)
    for j in range(128):
        for a in range(4):
            k = 2 * j - 1 + a
            if 0 <= k < 256:
                table[k, j] = stencil_weights[a]
    table[255, 128] = stencil_weights[0]
    table[0, 255] = stencil_weights[3]
    return table


def band_halo(width, right, left):
    table = np.zeros((128, 256), np.float32)
    for j in range(width // 2):
        for a in range(4):
            k = 2 * j - 1 + a
            if 0 <= k < width:
                table[right + k, j] = stencil_weights[a]
        for a in range(4):
            k = -3 - 2 * j + a
            if -width <= k < 0:
                table[left + k, 127 - j] = stencil_weights[a]
    table[left - 1, 128] = stencil_weights[0]
    table[right, 255] = stencil_weights[3]
    return table


def lane_iota(shape):
    return lax.broadcasted_iota(jnp.int32, shape, 1)


def words_wide(words):
    return jnp.concatenate([words, words], axis=0).T


def land_mask(wide, tile):
    lane = lane_iota(wide.shape)
    place = 4 * tile + lax.shift_right_logical(lane, 5)
    word = jnp.take_along_axis(wide, place, axis=1, mode="promise_in_bounds")
    return (word & lax.shift_left(jnp.int32(1), lane & 31)) != 0


def split(x):
    high = x.astype(bf16)
    low = (x - high.astype(f32)).astype(bf16)
    return high, low


def dot(a, b):
    return jnp.dot(a, b, preferred_element_type=f32)


def down_rows(line, count):
    return jnp.broadcast_to(line, (128, 128)).T[0:count]


def rows_down(ref, start, count, *rest):
    index = lambda a: (*rest, pl.ds(start + a, count, stride=2), slice(None))
    outer = ref[index(0)] + ref[index(3)]
    inner = ref[index(1)] + ref[index(2)]
    return stencil_weights[0] * outer + stencil_weights[1] * inner


def on_chip(x):
    return pltpu.with_memory_space_constraint(x, pltpu.VMEM)


def in_hbm(x):
    return pltpu.with_memory_space_constraint(x, pltpu.HBM)


def columns_kernel(
    place_ref, field_ref, words_ref,
    to_left_ref, to_right_ref, near_ref, near_words_ref, cos_ref,
    left_ref, right_ref, sems,
    *, total_rows,
):
    rows, cols = field_ref.shape
    small = [
        pltpu.make_async_copy(words_ref, near_words_ref, sems.at[0]),
        pltpu.make_async_copy(field_ref.at[:, 0:128], left_ref, sems.at[1]),
        pltpu.make_async_copy(field_ref.at[:, cols - 128 : cols], right_ref, sems.at[2]),
    ]
    quarter = rows // 4
    large = [
        pltpu.make_async_copy(
            field_ref.at[k * quarter : k * quarter + quarter, :],
            near_ref.at[k * quarter : k * quarter + quarter, :],
            sems.at[3 + k],
        )
        for k in range(4)
    ]
    for copy in small + large:
        copy.start()
    line = lax.broadcasted_iota(jnp.int32, (8, 128), 0)
    lane = lane_iota((8, 128))
    around = jnp.where(lane < 16, lane - 16, rows + lane - 16)
    global_rows = place_ref[0] * rows + jnp.where(line < rows // 128, line * 128 + lane, around)
    latitude = ((global_rows.astype(f32) + 0.5) / total_rows - 0.5) * math.pi
    inside = (global_rows >= 0) & (global_rows < total_rows)
    cos_ref[...] = jnp.where(inside, jnp.cos(latitude), 0.0)
    for copy in small:
        copy.wait()
    wide = words_wide(near_words_ref[...])
    left_mask = land_mask(wide, 0)
    right_mask = land_mask(wide, 15)
    lane = lane_iota(left_mask.shape)
    left_land = pltpu.roll(jnp.where(left_mask, 1.0, 0.0), 16, 1)
    right_land = pltpu.roll(jnp.where(right_mask, 1.0, 0.0), 112, 1)
    left_side = jnp.where(lane < 16, jnp.where(left_mask, left_ref[...], 0.0), left_land)
    right_side = jnp.where(lane >= 112, jnp.where(right_mask, right_ref[...], 0.0), right_land)
    both = jnp.where(lane < 64, left_side, right_side).T
    to_left_ref[...] = both[0:32]
    to_right_ref[...] = both[96:128]
    for copy in large:
        copy.wait()


def columns_strips(place, field, words, total_rows):
    rows, cols = field.shape
    return pl.pallas_call(
        functools.partial(columns_kernel, total_rows=total_rows),
        in_specs=[pl.BlockSpec(memory_space=pltpu.SMEM)] + [pl.BlockSpec(memory_space=pl.ANY)] * 2,
        out_specs=[pl.BlockSpec(memory_space=pltpu.VMEM)] * 5,
        out_shape=[
            pltpu.VMEM((32, rows), f32),
            pltpu.VMEM((32, rows), f32),
            pltpu.VMEM((rows, cols), f32),
            pltpu.VMEM(words.shape, words.dtype),
            pltpu.VMEM((8, 128), f32),
        ],
        scratch_shapes=[
            pltpu.VMEM((rows, 128), f32),
            pltpu.VMEM((rows, 128), f32),
            pltpu.SemaphoreType.DMA((7,)),
        ],
        compiler_params=pltpu.CompilerParams(vmem_limit_bytes=vmem_limit),
        name="columns_strips",
    )(place, field, words)


def rows_kernel(
    after_ref, top_ref, bottom_ref, top_words_ref, bottom_words_ref, right_ref, left_ref,
    up_ref, down_ref, halo_ref,
):
    del after_ref
    rows = halo_ref.shape[0]
    for part in range(rows // 128):
        cols = slice(part * 128, part * 128 + 128)
        halo_ref[cols, :] = jnp.concatenate(
            [right_ref[:, cols], jnp.zeros((64, 128), f32), left_ref[:, cols]], axis=0
        ).T
    for field_ref, words_ref, out_ref, first in (
        (top_ref, top_words_ref, up_ref, 0),
        (bottom_ref, bottom_words_ref, down_ref, rows - 16),
    ):
        wide = words_wide(words_ref[...])
        wide = wide[0:16] if first == 0 else wide[112:128]
        for tile in range(16):
            lanes = slice(tile * 128, tile * 128 + 128)
            mask = land_mask(wide, tile)
            out_ref[0:16, lanes] = jnp.where(mask, field_ref[:, lanes], 0.0)
            out_ref[16:32, lanes] = jnp.where(mask, 1.0, 0.0)
        out_ref[0:16, 2048:2176] = halo_ref[first : first + 16, :]
        out_ref[16:32, 2048:2176] = jnp.zeros((16, 128), f32)


def rows_strips(after, field, words, from_right, from_left):
    rows, cols = field.shape
    last = rows // 16 - 1
    return pl.pallas_call(
        rows_kernel,
        grid=(1,),
        in_specs=[
            pl.BlockSpec(memory_space=pltpu.VMEM),
            pl.BlockSpec((16, cols), lambda i: (0, 0)),
            pl.BlockSpec((16, cols), lambda i: (last, 0)),
            pl.BlockSpec((64, 128), lambda i: (0, 0)),
            pl.BlockSpec((64, 128), lambda i: (0, rows // 128 - 1)),
            pl.BlockSpec(memory_space=pltpu.VMEM),
            pl.BlockSpec(memory_space=pltpu.VMEM),
        ],
        out_specs=[pl.BlockSpec(memory_space=pltpu.VMEM)] * 3,
        out_shape=[
            pltpu.VMEM((32, cols + 128), f32),
            pltpu.VMEM((32, cols + 128), f32),
            pltpu.VMEM((rows, 128), f32),
        ],
        compiler_params=pltpu.CompilerParams(vmem_limit_bytes=vmem_limit),
        name="rows_strips",
    )(after, field, field, words, words, from_right, from_left)


def own_kernel(
    after_ref, field_ref, words_ref, cos_ref, band_ref, num_ref, den_ref,
    product_ref, cover_ref, main_ref, edge_ref, sheet_ref,
    *, skip,
):
    del after_ref
    step = pl.program_id(0)
    blocks = pl.num_programs(0) - 1
    height = field_ref.shape[0]

    @pl.when(step == 0)
    def _():
        sheet_ref[:, :, 0:24, :] = jnp.zeros((2, 9, 24, 128), f32)
        sheet_ref[:, :, 24 + 2 * height :, :] = jnp.zeros(
            (2, 9, sheet_ref.shape[2] - 24 - 2 * height, 128), f32
        )

    @pl.when(step < blocks)
    def _():
        wide = words_wide(words_ref[...])
        for tile in range(8):
            part = slice(tile * height, tile * height + height)
            for half in range(2):
                lanes = slice(tile * 256 + half * 128, tile * 256 + half * 128 + 128)
                mask = land_mask(wide, 2 * tile + half)
                high, low = split(jnp.where(mask, field_ref[:, lanes], 0.0))
                product_ref[part, half * 128 : half * 128 + 128] = high
                product_ref[part, 256 + half * 128 : 384 + half * 128] = low
                cover_ref[part, half * 128 : half * 128 + 128] = jnp.where(mask, 1.0, 0.0).astype(
                    bf16
                )
        cos = down_rows(cos_ref[pl.ds(skip + step, 1), :], 128)
        low_half = lane_iota((height, 128)) < 64
        start = pl.multiple_of(24 + step * height, 8)
        for which, (lhs_ref, depth) in enumerate(((product_ref, 512), (cover_ref, 256))):
            across = dot(lhs_ref[...], band_ref[0:depth, :])
            main_ref[...] = across[:, 0:128]
            edge_ref[...] = across[:, 128:256]
            zero = jnp.zeros((height, 128), f32)
            for t in range(9):
                get = lambda ref, k: ref[k * height : k * height + height, :]
                main = get(main_ref, t) if t < 8 else zero
                before = get(edge_ref, t - 1) if t > 0 else zero
                after = get(edge_ref, (t + 1) % 9) if t != 7 else zero
                sheet_ref[which, t, pl.ds(start, height), :] = (
                    main + jnp.where(low_half, before, after)
                ) * cos

    def down(count):
        first = 7 + step * height
        place = pl.multiple_of(step * (height // 2), 8)
        for which, out_ref in ((0, num_ref), (1, den_ref)):
            for t in range(9):
                out_ref[pl.ds(place, count), t * 128 : t * 128 + 128] = rows_down(
                    sheet_ref, first, count, which, t
                )

    @pl.when(step < blocks)
    def _():
        down(height // 2)

    @pl.when(step == blocks)
    def _():
        down(16)


def own_level(after, field, words, cosines, band, part):
    rows, cols = field.shape
    height = 128
    blocks = rows // 2 // height
    skip = part * blocks
    out = pltpu.VMEM((blocks * height // 2 + 16, cols // 2 + 128), f32)
    out_spec = pl.BlockSpec(memory_space=pltpu.VMEM)
    at = lambda b: skip + jnp.minimum(b, blocks - 1)
    return pl.pallas_call(
        functools.partial(own_kernel, skip=skip),
        grid=(blocks + 1,),
        in_specs=[
            pl.BlockSpec(memory_space=pl.ANY if part == 0 else pltpu.VMEM),
            pl.BlockSpec((height, cols), lambda b: (at(b), 0)),
            pl.BlockSpec((64, height), lambda b: (0, at(b))),
            pl.BlockSpec((8, 128), lambda b: (0, 0)),
            pl.BlockSpec((512, 256), lambda b: (0, 0)),
        ],
        out_specs=[out_spec, out_spec],
        out_shape=[out, out],
        scratch_shapes=[
            pltpu.VMEM((8 * height, 512), bf16),
            pltpu.VMEM((8 * height, 256), bf16),
            pltpu.VMEM((8 * height, 128), f32),
            pltpu.VMEM((8 * height, 128), f32),
            pltpu.VMEM((2, 9, 24 + (blocks + 1) * height, 128), f32),
        ],
        compiler_params=pltpu.CompilerParams(vmem_limit_bytes=vmem_limit),
        name="own_level",
    )(after, field, words, cosines, band)


def fold(x):
    return x.reshape(x.shape[0] // 8, 8, 128)


def levels_kernel(
    place_ref, num_a_ref, den_a_ref, num_b_ref, den_b_ref, halo_ref, top_ref, bottom_ref, cos_ref,
    band_ref, band_halo_ref, band_mixed_ref,
    one_ref, two_ref, three_ref, four_ref, stats_ref,
    p1_ref, c1_ref, p2_ref, c2_ref, p3_ref, c3_ref, tall_ref, strip_ref, value_ref,
    *, last_place,
):
    rows = halo_ref.shape[0]
    band = band_ref[...]

    def pick(before, after):
        shape = before.shape
        return jnp.where(lane_iota(shape) < 64, before, after)

    mixed = band_mixed_ref[...]
    tall_ref[:, 0:8, :] = jnp.zeros((4, 8, 128), f32)
    tall_ref[:, 8 + rows + 32 :, :] = jnp.zeros((4, 8, 128), f32)
    ends_cos = down_rows(cos_ref[4:5, :], 32)
    cos_top = ends_cos[0:16]
    cos_bottom = ends_cos[16:32]
    parts = [(0, 16, top_ref[0:16, 2048:2176], cos_top)]
    for k in range(rows // 128):
        part = halo_ref[k * 128 : k * 128 + 128, :]
        parts.append((16 + k * 128, 128, part, down_rows(cos_ref[k : k + 1, :], 128)))
    parts.append((16 + rows, 16, bottom_ref[0:16, 2048:2176], cos_bottom))
    for first, count, source, cos in parts:
        high, low = split(source)
        across = dot(high, mixed) + dot(low, mixed)
        for k in range(4):
            tall_ref[k, 8 + first : 8 + first + count, :] = (
                across[:, k * 128 : k * 128 + 128] * cos
            )
    count = rows // 2 + 16
    add_p, edge_p, add_c, edge_c = (rows_down(tall_ref, 7, count, k) for k in range(4))
    last = 7 * 128
    mid = rows // 4
    for a_ref, b_ref, out_ref, add, edge in (
        (num_a_ref, num_b_ref, p1_ref, add_p, edge_p),
        (den_a_ref, den_b_ref, c1_ref, add_c, edge_c),
    ):
        lower = lane_iota(edge.shape) < 64
        out_ref[0:mid, :] = a_ref[0:mid, :]
        out_ref[mid : mid + 16, :] = a_ref[mid : mid + 16, :] + b_ref[0:16, :]
        out_ref[mid + 16 : count, :] = b_ref[16 : mid + 16, :]
        out_ref[:, 0:128] = out_ref[:, 0:128] + jnp.where(lower, edge, 0.0)
        out_ref[:, last : last + 128] = out_ref[:, last : last + 128] + jnp.where(
            lower, 0.0, edge
        )
        out_ref[:, 1024:1152] = out_ref[:, 1024:1152] + add

    strip_ref[...] = jnp.zeros(strip_ref.shape, f32)
    for side, (ref, cos, first) in enumerate(((top_ref, cos_top, 8), (bottom_ref, cos_bottom, 24))):
        lhs = []
        for t in range(8):
            high, low = split(ref[0:16, t * 256 : t * 256 + 256])
            lhs += [high, low, ref[16:32, t * 256 : t * 256 + 256].astype(bf16)]
        out = dot(jnp.concatenate(lhs, axis=0), band)
        for which in range(2):
            parts = []
            for t in range(8):
                base = t * 48
                if which == 0:
                    parts.append(out[base : base + 16] + out[base + 16 : base + 32])
                else:
                    parts.append(out[base + 32 : base + 48])
            zero = jnp.zeros((16, 128), f32)
            for t in range(9):
                main = parts[t][:, 0:128] if t < 8 else zero
                before = parts[t - 1][:, 128:256] if t > 0 else zero
                after = parts[(t + 1) % 9][:, 128:256] if t != 7 else zero
                strip_ref[side, which, t, first : first + 16, :] = (main + pick(before, after)) * cos
        where = slice(0, 16) if side == 0 else slice(rows // 2, rows // 2 + 16)
        for which, out_ref in ((0, p1_ref), (1, c1_ref)):
            for t in range(9):
                lanes = slice(t * 128, t * 128 + 128)
                extra = rows_down(strip_ref, 7, 16, side, which, t)
                out_ref[where, lanes] = out_ref[where, lanes] + extra

    at_first = (place_ref[0] == 0).astype(jnp.int32)
    at_last = (place_ref[0] == last_place).astype(jnp.int32)
    sums = []

    def finish(num, den, halo, own):
        value = num / jnp.maximum(den, floor_value)
        row = lax.broadcasted_iota(jnp.int32, num.shape, 0)
        inside = (row >= halo * at_first) & (row < own + halo + (1 - at_last) * 4096)
        cover = jnp.where(inside, den, 0.0)
        return value, cover * value, cover

    level_one_sums = None
    for t in range(9):
        lanes = slice(t * 128, t * 128 + 128)
        value, product, cover = finish(p1_ref[:, lanes], c1_ref[:, lanes], 8, rows // 2)
        p1_ref[:, lanes] = product
        c1_ref[:, lanes] = cover
        if t < 8:
            own = slice(8, 8 + rows // 2)
            one_ref[:, lanes] = value[own]
            new = (
                jnp.sum(fold(product[own]), 0),
                jnp.sum(fold(cover[own]), 0),
                jnp.max(fold(value[own]), 0),
            )
            if level_one_sums is None:
                level_one_sums = new
            else:
                old = level_one_sums
                level_one_sums = (
                    old[0] + new[0], old[1] + new[1], jnp.maximum(old[2], new[2])
                )
    sums.append(level_one_sums)

    def next_level(p_ref, c_ref, tiles, in_rows, out_rows, halo, own_rows, out_ref, p_out, c_out):
        total = None
        nums = []
        dens = []
        for ref, dest in ((p_ref, nums), (c_ref, dens)):
            blocks = []
            for t in range(tiles):
                high, low = split(ref[:, t * 256 : t * 256 + 256])
                blocks.append(dot(high, band) + dot(low, band))
            high, low = split(ref[:, tiles * 256 : tiles * 256 + 128])
            ring = band_halo_ref[...]
            blocks.append(dot(high, ring) + dot(low, ring))
            count = tiles + 1
            for t in range(count):
                across = blocks[t][:, 0:128] + pick(
                    blocks[(t - 1) % count][:, 128:256], blocks[(t + 1) % count][:, 128:256]
                )
                slot = t % 4
                tall_ref[slot, 8 : 8 + in_rows, :] = across
                tall_ref[slot, 8 + in_rows : 2 * out_rows + 16, :] = jnp.zeros(
                    (2 * out_rows + 8 - in_rows, 128), f32
                )
                dest.append(rows_down(tall_ref, 7, out_rows, slot))
        for t in range(tiles + 1):
            value, product, cover = finish(nums[t], dens[t], halo, own_rows)
            if p_out is not None:
                p_out[:, t * 128 : t * 128 + 128] = product
                c_out[:, t * 128 : t * 128 + 128] = cover
            if t < tiles:
                own = slice(halo, halo + own_rows)
                value_ref[0, 0:out_rows, :] = value
                value_ref[1, 0:out_rows, :] = product
                value_ref[2, 0:out_rows, :] = cover
                v, p, c = (value_ref[k, own, :] for k in range(3))
                out_ref[:, t * 128 : t * 128 + 128] = v
                new = (jnp.sum(fold(p), 0), jnp.sum(fold(c), 0), jnp.max(fold(v), 0))
                total = (
                    new
                    if total is None
                    else (total[0] + new[0], total[1] + new[1], jnp.maximum(total[2], new[2]))
                )
        sums.append(total)

    next_level(p1_ref, c1_ref, 4, 272, 136, 4, 128, two_ref, p2_ref, c2_ref)
    next_level(p2_ref, c2_ref, 2, 136, 72, 2, 64, three_ref, p3_ref, c3_ref)
    next_level(p3_ref, c3_ref, 1, 72, 40, 1, 32, four_ref, None, None)

    lane = lane_iota((1, 128))
    row = jnp.zeros((1, 128), f32)
    for level in range(4):
        for kind in range(3):
            part = sums[level][kind]
            one = (jnp.max if kind == 2 else jnp.sum)(part, axis=0, keepdims=True)
            one = (jnp.max if kind == 2 else jnp.sum)(one, axis=1, keepdims=True)
            row = jnp.where(lane == kind * 4 + level, one, row)
    stats_ref[...] = jnp.broadcast_to(row, stats_ref.shape)


def all_levels(place, last_place, chips, owns, halo, top, bottom, cosines, tables, rows, cols):
    vmem = pl.BlockSpec(memory_space=pltpu.VMEM)
    outs = [jax.ShapeDtypeStruct((rows >> k, cols >> k), f32) for k in (1, 2, 3, 4)]
    half = rows // 2 + 16
    return pl.pallas_call(
        functools.partial(levels_kernel, last_place=last_place),
        in_specs=[pl.BlockSpec(memory_space=pltpu.SMEM)] + [vmem] * 11,
        out_specs=[vmem] * 5,
        out_shape=outs + [pltpu.VMEM((chips, 128), f32)],
        scratch_shapes=[
            pltpu.VMEM((half, cols // 2 + 128), f32),
            pltpu.VMEM((half, cols // 2 + 128), f32),
            pltpu.VMEM((136, cols // 4 + 128), f32),
            pltpu.VMEM((136, cols // 4 + 128), f32),
            pltpu.VMEM((72, cols // 8 + 128), f32),
            pltpu.VMEM((72, cols // 8 + 128), f32),
            pltpu.VMEM((4, rows + 48, 128), f32),
            pltpu.VMEM((2, 2, 9, 48, 128), f32),
            pltpu.VMEM((3, 136, 128), f32),
        ],
        compiler_params=pltpu.CompilerParams(vmem_limit_bytes=vmem_limit),
        name="all_levels",
    )(place, *owns, halo, top, bottom, cosines, *tables)


def per_device(surface_field, land_words):
    rows, cols = surface_field.shape
    row_devices = lax.axis_size(ROWS)
    col_devices = lax.axis_size(COLS)
    total_rows = rows * row_devices
    position = lax.axis_index(ROWS)

    band = jnp.asarray(band_main(), bf16)
    ring = jnp.asarray(band_halo(64, 0, 128), bf16)
    mixed = jnp.asarray(
        np.concatenate([band_halo(16, 0, 128), band_halo(16, 16, 112)], axis=1), bf16
    )

    place = jnp.reshape(position, (1,))
    words = land_words.T

    east = [(i, (i + 1) % col_devices) for i in range(col_devices)]
    west = [(target, source) for source, target in east]
    south = [(i, i + 1) for i in range(row_devices - 1)]
    north = [(target, source) for source, target in south]

    to_left, to_right, near, near_words, cosines = columns_strips(
        place, in_hbm(surface_field), in_hbm(words), total_rows
    )
    near, near_words, cosines = on_chip(near), on_chip(near_words), on_chip(cosines)
    from_right = lax.ppermute(to_left, COLS, west)
    from_left = lax.ppermute(to_right, COLS, east)
    twice = jnp.concatenate([band, band], axis=0)
    upper = own_level(band, near, near_words, cosines, twice, 0)
    to_up, to_down, halo = rows_strips(on_chip(upper[0]), near, near_words, on_chip(from_right), on_chip(from_left))
    bottom = lax.ppermute(to_up, ROWS, north)
    top = lax.ppermute(to_down, ROWS, south)
    lower = own_level(on_chip(halo), near, near_words, cosines, twice, 1)
    chips = lax.axis_size(CHIPS)
    one, two, three, four, stats = all_levels(
        place, row_devices - 1, chips, [on_chip(x) for x in (*upper, *lower)],
        on_chip(halo), on_chip(top), on_chip(bottom), cosines, (band, ring, mixed), rows, cols,
    )

    is_sum = jnp.arange(128) < 8
    every = lax.all_to_all(stats, CHIPS, 0, 0, tiled=True)
    stats = jnp.where(is_sum, jnp.sum(every, axis=0), jnp.max(every, axis=0))
    other = lax.ppermute(stats, CORE, [(0, 1), (1, 0)])
    sums = stats[0:8] + other[0:8]
    maxima = jnp.maximum(stats[8:12], other[8:12])
    means = sums[0:4] / (sums[4:8] + mean_eps)
    return (one, two, three, four, means, maxima)


def solution(mesh):
    finer = Mesh(
        mesh.devices.reshape(2, 4, 2, 2, 4), ("rows_0", "rows_1", "rows_2", "cols_0", "cols_1")
    )
    in_specs = (P(ROWS, COLS), P(ROWS, COLS))
    out_specs = (P(ROWS, COLS), P(ROWS, COLS), P(ROWS, COLS), P(ROWS, COLS), P(), P())
    return jax.shard_map(
        per_device, mesh=finer, in_specs=in_specs, out_specs=out_specs, check_vma=False
    )
```

```python
import functools
import math

import jax
import jax.numpy as jnp
import numpy as np
from jax import lax
from jax.experimental import pallas as pl
from jax.experimental.pallas import tpu as pltpu
from jax.sharding import Mesh
from jax.sharding import PartitionSpec as P

ROWS = ("rows_0", "rows_1", "rows_2")
COLS = ("cols_0", "cols_1")
CHIPS = ("rows_0", "rows_1", "cols_0", "cols_1")
CORE = "rows_2"


stencil_weights = (0.125, 0.375, 0.375, 0.125)
floor_value = 0.05
mean_eps = 1e-06

vmem_limit = 20 * 1024 * 1024

f32 = jnp.float32
bf16 = jnp.bfloat16


def band_main():
    table = np.zeros((256, 256), np.float32)
    for j in range(128):
        for a in range(4):
            k = 2 * j - 1 + a
            if 0 <= k < 256:
                table[k, j] = stencil_weights[a]
    table[255, 128] = stencil_weights[0]
    table[0, 255] = stencil_weights[3]
    return table


def band_halo(width, right, left):
    table = np.zeros((128, 256), np.float32)
    for j in range(width // 2):
        for a in range(4):
            k = 2 * j - 1 + a
            if 0 <= k < width:
                table[right + k, j] = stencil_weights[a]
        for a in range(4):
            k = -3 - 2 * j + a
            if -width <= k < 0:
                table[left + k, 127 - j] = stencil_weights[a]
    table[left - 1, 128] = stencil_weights[0]
    table[right, 255] = stencil_weights[3]
    return table


def lane_iota(shape):
    return lax.broadcasted_iota(jnp.int32, shape, 1)


def words_wide(words):
    return jnp.concatenate([words, words], axis=0).T


def land_mask(wide, tile):
    lane = lane_iota(wide.shape)
    place = 4 * tile + lax.shift_right_logical(lane, 5)
    word = jnp.take_along_axis(wide, place, axis=1, mode="promise_in_bounds")
    return (word & lax.shift_left(jnp.int32(1), lane & 31)) != 0


def split(x):
    high = x.astype(bf16)
    low = (x - high.astype(f32)).astype(bf16)
    return high, low


def dot(a, b):
    return jnp.dot(a, b, preferred_element_type=f32)


def down_rows(line, count):
    return jnp.broadcast_to(line, (128, 128)).T[0:count]


def rows_down(ref, start, count, *rest):
    index = lambda a: (*rest, pl.ds(start + a, count, stride=2), slice(None))
    outer = ref[index(0)] + ref[index(3)]
    inner = ref[index(1)] + ref[index(2)]
    return stencil_weights[0] * outer + stencil_weights[1] * inner


def on_chip(x):
    return pltpu.with_memory_space_constraint(x, pltpu.VMEM)


def in_hbm(x):
    return pltpu.with_memory_space_constraint(x, pltpu.HBM)


def columns_kernel(
    place_ref, field_ref, words_ref,
    to_left_ref, to_right_ref, near_ref, near_words_ref, cos_ref,
    left_ref, right_ref, sems,
    *, total_rows,
):
    rows, cols = field_ref.shape
    small = [
        pltpu.make_async_copy(words_ref, near_words_ref, sems.at[0]),
        pltpu.make_async_copy(field_ref.at[:, 0:128], left_ref, sems.at[1]),
        pltpu.make_async_copy(field_ref.at[:, cols - 128 : cols], right_ref, sems.at[2]),
    ]
    quarter = rows // 4
    large = [
        pltpu.make_async_copy(
            field_ref.at[k * quarter : k * quarter + quarter, :],
            near_ref.at[k * quarter : k * quarter + quarter, :],
            sems.at[3 + k],
        )
        for k in range(4)
    ]
    for copy in small + large:
        copy.start()
    line = lax.broadcasted_iota(jnp.int32, (8, 128), 0)
    lane = lane_iota((8, 128))
    around = jnp.where(lane < 16, lane - 16, rows + lane - 16)
    global_rows = place_ref[0] * rows + jnp.where(line < rows // 128, line * 128 + lane, around)
    latitude = ((global_rows.astype(f32) + 0.5) / total_rows - 0.5) * math.pi
    inside = (global_rows >= 0) & (global_rows < total_rows)
    cos_ref[...] = jnp.where(inside, jnp.cos(latitude), 0.0)
    for copy in small:
        copy.wait()
    wide = words_wide(near_words_ref[...])
    left_mask = land_mask(wide, 0)
    right_mask = land_mask(wide, 15)
    lane = lane_iota(left_mask.shape)
    left_land = pltpu.roll(jnp.where(left_mask, 1.0, 0.0), 16, 1)
    right_land = pltpu.roll(jnp.where(right_mask, 1.0, 0.0), 112, 1)
    left_side = jnp.where(lane < 16, jnp.where(left_mask, left_ref[...], 0.0), left_land)
    right_side = jnp.where(lane >= 112, jnp.where(right_mask, right_ref[...], 0.0), right_land)
    both = jnp.where(lane < 64, left_side, right_side).T
    to_left_ref[...] = both[0:32]
    to_right_ref[...] = both[96:128]
    for copy in large:
        copy.wait()


def columns_strips(place, field, words, total_rows):
    rows, cols = field.shape
    return pl.pallas_call(
        functools.partial(columns_kernel, total_rows=total_rows),
        in_specs=[pl.BlockSpec(memory_space=pltpu.SMEM)] + [pl.BlockSpec(memory_space=pl.ANY)] * 2,
        out_specs=[pl.BlockSpec(memory_space=pltpu.VMEM)] * 5,
        out_shape=[
            pltpu.VMEM((32, rows), f32),
            pltpu.VMEM((32, rows), f32),
            pltpu.VMEM((rows, cols), f32),
            pltpu.VMEM(words.shape, words.dtype),
            pltpu.VMEM((8, 128), f32),
        ],
        scratch_shapes=[
            pltpu.VMEM((rows, 128), f32),
            pltpu.VMEM((rows, 128), f32),
            pltpu.SemaphoreType.DMA((7,)),
        ],
        compiler_params=pltpu.CompilerParams(vmem_limit_bytes=vmem_limit),
        name="columns_strips",
    )(place, field, words)


def rows_kernel(
    place_ref, after_ref, field_ref, words_ref, right_ref, left_ref,
    to_core_ref, to_chip_ref, halo_ref, wide_ref,
):
    del after_ref
    rows = halo_ref.shape[0]
    for part in range(rows // 128):
        cols = slice(part * 128, part * 128 + 128)
        halo_ref[cols, :] = jnp.concatenate(
            [right_ref[:, cols], jnp.zeros((64, 128), f32), left_ref[:, cols]], axis=0
        ).T
    odd = place_ref[0] & 1
    for out_ref, bottom in ((to_core_ref, 1 - odd), (to_chip_ref, odd)):
        first = pl.multiple_of(bottom * (rows - 16), 16)
        wide_ref[...] = words_wide(words_ref[:, pl.ds(pl.multiple_of(bottom * (rows - 128), 128), 128)])
        wide = wide_ref[pl.ds(pl.multiple_of(bottom * 112, 16), 16), :]
        for tile in range(16):
            lanes = slice(tile * 128, tile * 128 + 128)
            mask = land_mask(wide, tile)
            out_ref[0:16, lanes] = jnp.where(mask, field_ref[pl.ds(first, 16), lanes], 0.0)
            out_ref[16:32, lanes] = jnp.where(mask, 1.0, 0.0)
        out_ref[0:16, 2048:2176] = halo_ref[pl.ds(first, 16), :]
        out_ref[16:32, 2048:2176] = jnp.zeros((16, 128), f32)


def rows_strips(place, after, field, words, from_right, from_left):
    rows, cols = field.shape
    return pl.pallas_call(
        rows_kernel,
        in_specs=[pl.BlockSpec(memory_space=pltpu.SMEM)]
        + [pl.BlockSpec(memory_space=pltpu.VMEM)] * 5,
        out_specs=[pl.BlockSpec(memory_space=pltpu.VMEM)] * 3,
        out_shape=[
            pltpu.VMEM((32, cols + 128), f32),
            pltpu.VMEM((32, cols + 128), f32),
            pltpu.VMEM((rows, 128), f32),
        ],
        scratch_shapes=[pltpu.VMEM((128, 128), jnp.int32)],
        compiler_params=pltpu.CompilerParams(vmem_limit_bytes=vmem_limit),
        name="rows_strips",
    )(place, after, field, words, from_right, from_left)


def side_terms(halo_ref, cos_ref, mixed_ref, side_ref, tall_ref):
    rows = halo_ref.shape[0]
    tall_ref[:, 0:24, :] = jnp.zeros((4, 24, 128), f32)
    tall_ref[:, 24 + rows :, :] = jnp.zeros((4, 24, 128), f32)
    mixed = mixed_ref[...]
    for part in range(rows // 128):
        high, low = split(halo_ref[part * 128 : part * 128 + 128, :])
        across = dot(high, mixed) + dot(low, mixed)
        cos = down_rows(cos_ref[part : part + 1, :], 128)
        for k in range(4):
            tall_ref[k, 24 + part * 128 : 152 + part * 128, :] = (
                across[:, k * 128 : k * 128 + 128] * cos
            )
    for k in range(4):
        side_ref[k] = rows_down(tall_ref, 7, side_ref.shape[1], k)


def lower_kernel(
    halo_ref, mixed_ref, field_ref, words_ref, cos_ref, band_ref,
    num_ref, den_ref, side_ref, *scratch, skip,
):
    @pl.when(pl.program_id(0) == 0)
    def _():
        side_terms(halo_ref, cos_ref, mixed_ref, side_ref, scratch[-1])

    upper_kernel(field_ref, words_ref, cos_ref, band_ref, num_ref, den_ref, *scratch[:-1], skip=skip)


def upper_kernel(
    field_ref, words_ref, cos_ref, band_ref, num_ref, den_ref,
    product_ref, cover_ref, main_ref, edge_ref, sheet_ref,
    *, skip,
):
    step = pl.program_id(0)
    blocks = pl.num_programs(0) - 1
    height = field_ref.shape[0]

    @pl.when(step == 0)
    def _():
        sheet_ref[:, :, 0:24, :] = jnp.zeros((2, 9, 24, 128), f32)
        sheet_ref[:, :, 24 + 2 * height :, :] = jnp.zeros(
            (2, 9, sheet_ref.shape[2] - 24 - 2 * height, 128), f32
        )

    @pl.when(step < blocks)
    def _():
        wide = words_wide(words_ref[...])
        for tile in range(8):
            part = slice(tile * height, tile * height + height)
            for half in range(2):
                lanes = slice(tile * 256 + half * 128, tile * 256 + half * 128 + 128)
                mask = land_mask(wide, 2 * tile + half)
                high, low = split(jnp.where(mask, field_ref[:, lanes], 0.0))
                product_ref[part, half * 128 : half * 128 + 128] = high
                product_ref[part, 256 + half * 128 : 384 + half * 128] = low
                cover_ref[part, half * 128 : half * 128 + 128] = jnp.where(mask, 1.0, 0.0).astype(
                    bf16
                )
        cos = down_rows(cos_ref[pl.ds(skip + step, 1), :], 128)
        low_half = lane_iota((height, 128)) < 64
        start = pl.multiple_of(24 + step * height, 8)
        for which, (lhs_ref, depth) in enumerate(((product_ref, 512), (cover_ref, 256))):
            across = dot(lhs_ref[...], band_ref[0:depth, :])
            main_ref[...] = across[:, 0:128]
            edge_ref[...] = across[:, 128:256]
            zero = jnp.zeros((height, 128), f32)
            for t in range(9):
                get = lambda ref, k: ref[k * height : k * height + height, :]
                main = get(main_ref, t) if t < 8 else zero
                before = get(edge_ref, t - 1) if t > 0 else zero
                after = get(edge_ref, (t + 1) % 9) if t != 7 else zero
                sheet_ref[which, t, pl.ds(start, height), :] = (
                    main + jnp.where(low_half, before, after)
                ) * cos

    def down(count):
        first = 7 + step * height
        place = pl.multiple_of(step * (height // 2), 8)
        for which, out_ref in ((0, num_ref), (1, den_ref)):
            for t in range(9):
                out_ref[pl.ds(place, count), t * 128 : t * 128 + 128] = rows_down(
                    sheet_ref, first, count, which, t
                )

    @pl.when(step < blocks)
    def _():
        down(height // 2)

    @pl.when(step == blocks)
    def _():
        down(16)


def own_level(field, words, cosines, band, part, *beside):
    rows, cols = field.shape
    height = 128
    blocks = rows // 2 // height
    skip = part * blocks
    vmem = pl.BlockSpec(memory_space=pltpu.VMEM)
    half = pltpu.VMEM((blocks * height // 2 + 16, cols // 2 + 128), f32)
    side = [pltpu.VMEM((4, rows // 2 + 16, 128), f32)] if beside else []
    tall = [pltpu.VMEM((4, rows + 48, 128), f32)] if beside else []
    at = lambda b: skip + jnp.minimum(b, blocks - 1)
    return pl.pallas_call(
        functools.partial(lower_kernel if beside else upper_kernel, skip=skip),
        grid=(blocks + 1,),
        in_specs=[vmem] * len(beside)
        + [
            pl.BlockSpec((height, cols), lambda b: (at(b), 0)),
            pl.BlockSpec((64, height), lambda b: (0, at(b))),
            pl.BlockSpec((8, 128), lambda b: (0, 0)),
            pl.BlockSpec((512, 256), lambda b: (0, 0)),
        ],
        out_specs=[vmem] * (2 + len(side)),
        out_shape=[half, half] + side,
        scratch_shapes=[
            pltpu.VMEM((8 * height, 512), bf16),
            pltpu.VMEM((8 * height, 256), bf16),
            pltpu.VMEM((8 * height, 128), f32),
            pltpu.VMEM((8 * height, 128), f32),
            pltpu.VMEM((2, 9, 24 + (blocks + 1) * height, 128), f32),
        ]
        + tall,
        compiler_params=pltpu.CompilerParams(vmem_limit_bytes=vmem_limit),
        name="own_level",
    )(*beside, field, words, cosines, band)


def fold(x):
    return x.reshape(x.shape[0] // 8, 8, 128)


def levels_kernel(
    place_ref, num_a_ref, den_a_ref, num_b_ref, den_b_ref, side_ref, core_ref, chip_ref, cos_ref,
    band_ref, band_halo_ref, band_mixed_ref,
    one_out, two_out, three_out, four_out, stats_ref,
    one_ref, two_ref, three_ref, four_ref, sems,
    p1_ref, c1_ref, p2_ref, c2_ref, p3_ref, c3_ref, tall_ref, strip_ref, value_ref,
    *, last_place,
):
    count = side_ref.shape[1]
    rows = 2 * (count - 16)
    band = band_ref[...]
    mixed = band_mixed_ref[...]
    odd = (place_ref[0] & 1) == 1
    tall_ref[:, 0:8, :] = jnp.zeros((4, 8, 128), f32)

    def pick(before, after):
        shape = before.shape
        return jnp.where(lane_iota(shape) < 64, before, after)

    last = 7 * 128
    add_p, edge_p, add_c, edge_c = (side_ref[k] for k in range(4))
    mid = rows // 4
    for a_ref, b_ref, out_ref, add, edge in (
        (num_a_ref, num_b_ref, p1_ref, add_p, edge_p),
        (den_a_ref, den_b_ref, c1_ref, add_c, edge_c),
    ):
        lower = lane_iota(edge.shape) < 64
        out_ref[0:mid, :] = a_ref[0:mid, :]
        out_ref[mid : mid + 16, :] = a_ref[mid : mid + 16, :] + b_ref[0:16, :]
        out_ref[mid + 16 : count, :] = b_ref[16 : mid + 16, :]
        out_ref[:, 0:128] = out_ref[:, 0:128] + jnp.where(lower, edge, 0.0)
        out_ref[:, last : last + 128] = out_ref[:, last : last + 128] + jnp.where(
            lower, 0.0, edge
        )
        out_ref[:, 1024:1152] = out_ref[:, 1024:1152] + add

    strip_ref[...] = jnp.zeros(strip_ref.shape, f32)
    ends_cos = down_rows(cos_ref[4:5, :], 32)
    for side, (cos, first) in enumerate(((ends_cos[0:16], 8), (ends_cos[16:32], 24))):
        of_core = odd if side == 0 else jnp.logical_not(odd)
        strip = jnp.where(of_core, core_ref[...], chip_ref[...])
        lhs = []
        for t in range(8):
            high, low = split(strip[0:16, t * 256 : t * 256 + 256])
            lhs += [high, low, strip[16:32, t * 256 : t * 256 + 256].astype(bf16)]
        out = dot(jnp.concatenate(lhs, axis=0), band)
        high, low = split(strip[0:16, 2048:2176])
        corner = dot(high, mixed) + dot(low, mixed)
        for which in range(2):
            parts = []
            for t in range(8):
                base = t * 48
                if which == 0:
                    parts.append(out[base : base + 16] + out[base + 16 : base + 32])
                else:
                    parts.append(out[base + 32 : base + 48])
            parts.append(corner[:, which * 256 : which * 256 + 256])
            for t in range(9):
                edges = pick(parts[(t - 1) % 9][:, 128:256], parts[(t + 1) % 9][:, 128:256])
                strip_ref[side, which, t, first : first + 16, :] = (
                    parts[t][:, 0:128] + edges
                ) * cos
        where = slice(0, 16) if side == 0 else slice(rows // 2, rows // 2 + 16)
        for which, out_ref in ((0, p1_ref), (1, c1_ref)):
            for t in range(9):
                lanes = slice(t * 128, t * 128 + 128)
                extra = rows_down(strip_ref, 7, 16, side, which, t)
                out_ref[where, lanes] = out_ref[where, lanes] + extra

    at_first = (place_ref[0] == 0).astype(jnp.int32)
    at_last = (place_ref[0] == last_place).astype(jnp.int32)
    sums = []

    def finish(num, den, halo, own):
        value = num / jnp.maximum(den, floor_value)
        row = lax.broadcasted_iota(jnp.int32, num.shape, 0)
        inside = (row >= halo * at_first) & (row < own + halo + (1 - at_last) * 4096)
        cover = jnp.where(inside, den, 0.0)
        return value, cover * value, cover

    level_one_sums = None
    for t in range(9):
        lanes = slice(t * 128, t * 128 + 128)
        value, product, cover = finish(p1_ref[:, lanes], c1_ref[:, lanes], 8, rows // 2)
        p1_ref[:, lanes] = product
        c1_ref[:, lanes] = cover
        if t < 8:
            own = slice(8, 8 + rows // 2)
            one_ref[:, lanes] = value[own]
            new = (
                jnp.sum(fold(product[own]), 0),
                jnp.sum(fold(cover[own]), 0),
                jnp.max(fold(value[own]), 0),
            )
            if level_one_sums is None:
                level_one_sums = new
            else:
                old = level_one_sums
                level_one_sums = (
                    old[0] + new[0], old[1] + new[1], jnp.maximum(old[2], new[2])
                )
    sums.append(level_one_sums)
    writes = [
        pltpu.make_async_copy(source, target, sems.at[k])
        for k, (source, target) in enumerate(
            ((one_ref, one_out), (two_ref, two_out), (three_ref, three_out), (four_ref, four_out))
        )
    ]
    writes[0].start()

    def next_level(p_ref, c_ref, tiles, in_rows, out_rows, halo, own_rows, out_ref, p_out, c_out):
        total = None
        nums = []
        dens = []
        for ref, dest in ((p_ref, nums), (c_ref, dens)):
            blocks = []
            for t in range(tiles):
                high, low = split(ref[:, t * 256 : t * 256 + 256])
                blocks.append(dot(high, band) + dot(low, band))
            high, low = split(ref[:, tiles * 256 : tiles * 256 + 128])
            ring = band_halo_ref[...]
            blocks.append(dot(high, ring) + dot(low, ring))
            count = tiles + 1
            for t in range(count):
                across = blocks[t][:, 0:128] + pick(
                    blocks[(t - 1) % count][:, 128:256], blocks[(t + 1) % count][:, 128:256]
                )
                slot = t % 4
                tall_ref[slot, 8 : 8 + in_rows, :] = across
                tall_ref[slot, 8 + in_rows : 2 * out_rows + 16, :] = jnp.zeros(
                    (2 * out_rows + 8 - in_rows, 128), f32
                )
                dest.append(rows_down(tall_ref, 7, out_rows, slot))
        for t in range(tiles + 1):
            value, product, cover = finish(nums[t], dens[t], halo, own_rows)
            if p_out is not None:
                p_out[:, t * 128 : t * 128 + 128] = product
                c_out[:, t * 128 : t * 128 + 128] = cover
            if t < tiles:
                own = slice(halo, halo + own_rows)
                value_ref[0, 0:out_rows, :] = value
                value_ref[1, 0:out_rows, :] = product
                value_ref[2, 0:out_rows, :] = cover
                v, p, c = (value_ref[k, own, :] for k in range(3))
                out_ref[:, t * 128 : t * 128 + 128] = v
                new = (jnp.sum(fold(p), 0), jnp.sum(fold(c), 0), jnp.max(fold(v), 0))
                total = (
                    new
                    if total is None
                    else (total[0] + new[0], total[1] + new[1], jnp.maximum(total[2], new[2]))
                )
        sums.append(total)

    next_level(p1_ref, c1_ref, 4, 272, 136, 4, 128, two_ref, p2_ref, c2_ref)
    writes[1].start()
    next_level(p2_ref, c2_ref, 2, 136, 72, 2, 64, three_ref, p3_ref, c3_ref)
    writes[2].start()
    next_level(p3_ref, c3_ref, 1, 72, 40, 1, 32, four_ref, None, None)
    writes[3].start()

    lane = lane_iota((1, 128))
    row = jnp.zeros((1, 128), f32)
    for level in range(4):
        for kind in range(3):
            part = sums[level][kind]
            one = (jnp.max if kind == 2 else jnp.sum)(part, axis=0, keepdims=True)
            one = (jnp.max if kind == 2 else jnp.sum)(one, axis=1, keepdims=True)
            row = jnp.where(lane == kind * 4 + level, one, row)
    stats_ref[...] = jnp.broadcast_to(row, stats_ref.shape)
    for write in writes:
        write.wait()


def all_levels(place, last_place, chips, owns, by_core, by_chip, cosines, tables, rows, cols):
    vmem = pl.BlockSpec(memory_space=pltpu.VMEM)
    shapes = [(rows >> k, cols >> k) for k in (1, 2, 3, 4)]
    outs = [jax.ShapeDtypeStruct(shape, f32) for shape in shapes]
    half = rows // 2 + 16
    return pl.pallas_call(
        functools.partial(levels_kernel, last_place=last_place),
        in_specs=[pl.BlockSpec(memory_space=pltpu.SMEM)] + [vmem] * 11,
        out_specs=[pl.BlockSpec(memory_space=pl.ANY)] * 4 + [vmem],
        out_shape=outs + [pltpu.VMEM((chips, 128), f32)],
        scratch_shapes=[pltpu.VMEM(shape, f32) for shape in shapes]
        + [pltpu.SemaphoreType.DMA((4,))]
        + [
            pltpu.VMEM((half, cols // 2 + 128), f32),
            pltpu.VMEM((half, cols // 2 + 128), f32),
            pltpu.VMEM((136, cols // 4 + 128), f32),
            pltpu.VMEM((136, cols // 4 + 128), f32),
            pltpu.VMEM((72, cols // 8 + 128), f32),
            pltpu.VMEM((72, cols // 8 + 128), f32),
            pltpu.VMEM((4, rows + 48, 128), f32),
            pltpu.VMEM((2, 2, 9, 48, 128), f32),
            pltpu.VMEM((3, 136, 128), f32),
        ],
        compiler_params=pltpu.CompilerParams(vmem_limit_bytes=vmem_limit),
        name="all_levels",
    )(place, *owns, by_core, by_chip, cosines, *tables)


def per_device(surface_field, land_words):
    rows, cols = surface_field.shape
    row_devices = lax.axis_size(ROWS)
    col_devices = lax.axis_size(COLS)
    total_rows = rows * row_devices
    position = lax.axis_index(ROWS)

    band = jnp.asarray(band_main(), bf16)
    ring = jnp.asarray(band_halo(64, 0, 128), bf16)
    mixed = jnp.asarray(
        np.concatenate([band_halo(16, 0, 128), band_halo(16, 16, 112)], axis=1), bf16
    )

    place = jnp.reshape(position, (1,))
    words = land_words.T

    east = [(i, (i + 1) % col_devices) for i in range(col_devices)]
    west = [(target, source) for source, target in east]

    to_left, to_right, near, near_words, cosines = columns_strips(
        place, in_hbm(surface_field), in_hbm(words), total_rows
    )
    near, near_words, cosines = on_chip(near), on_chip(near_words), on_chip(cosines)
    from_right = lax.ppermute(to_left, COLS, west)
    from_left = lax.ppermute(to_right, COLS, east)
    twice = jnp.concatenate([band, band], axis=0)
    upper = own_level(near, near_words, cosines, twice, 0)
    to_core, to_chip, halo = rows_strips(
        place, on_chip(upper[0]), near, near_words, on_chip(from_right), on_chip(from_left)
    )
    by_core = lax.ppermute(to_core, ROWS, [(i, i ^ 1) for i in range(row_devices)])
    by_chip = lax.ppermute(to_chip, ROWS, [(i, ((i - 1) ^ 1) + 1) for i in range(1, row_devices - 1)])
    lower = own_level(near, near_words, cosines, twice, 1, on_chip(halo), mixed)
    chips = lax.axis_size(CHIPS)
    one, two, three, four, stats = all_levels(
        place, row_devices - 1, chips, [on_chip(x) for x in (*upper, *lower)],
        on_chip(by_core), on_chip(by_chip), cosines, (band, ring, mixed), rows, cols,
    )

    is_sum = jnp.arange(128) < 8
    every = lax.all_to_all(stats, CHIPS, 0, 0, tiled=True)
    stats = jnp.where(is_sum, jnp.sum(every, axis=0), jnp.max(every, axis=0))
    other = lax.ppermute(stats, CORE, [(0, 1), (1, 0)])
    sums = stats[0:8] + other[0:8]
    maxima = jnp.maximum(stats[8:12], other[8:12])
    means = sums[0:4] / (sums[4:8] + mean_eps)
    return (one, two, three, four, means, maxima)


def solution(mesh):
    finer = Mesh(
        mesh.devices.reshape(2, 4, 2, 2, 4), ("rows_0", "rows_1", "rows_2", "cols_0", "cols_1")
    )
    in_specs = (P(ROWS, COLS), P(ROWS, COLS))
    out_specs = (P(ROWS, COLS), P(ROWS, COLS), P(ROWS, COLS), P(ROWS, COLS), P(), P())
    return jax.shard_map(
        per_device, mesh=finer, in_specs=in_specs, out_specs=out_specs, check_vma=False
    )
```

```python
import functools
import math

import jax
import jax.numpy as jnp
import numpy as np
from jax import lax
from jax.experimental import pallas as pl
from jax.experimental.pallas import tpu as pltpu
from jax.sharding import Mesh
from jax.sharding import PartitionSpec as P

ROWS = ("rows_0", "rows_1", "rows_2")
COLS = ("cols_0", "cols_1")
CHIPS = ("rows_0", "rows_1", "cols_0", "cols_1")
CORE = "rows_2"


stencil_weights = (0.125, 0.375, 0.375, 0.125)
floor_value = 0.05
mean_eps = 1e-06

vmem_limit = 20 * 1024 * 1024

f32 = jnp.float32
bf16 = jnp.bfloat16


def band_main():
    table = np.zeros((256, 256), np.float32)
    for j in range(128):
        for a in range(4):
            k = 2 * j - 1 + a
            if 0 <= k < 256:
                table[k, j] = stencil_weights[a]
    table[255, 128] = stencil_weights[0]
    table[0, 255] = stencil_weights[3]
    return table


def band_halo(width, right, left):
    table = np.zeros((128, 256), np.float32)
    for j in range(width // 2):
        for a in range(4):
            k = 2 * j - 1 + a
            if 0 <= k < width:
                table[right + k, j] = stencil_weights[a]
        for a in range(4):
            k = -3 - 2 * j + a
            if -width <= k < 0:
                table[left + k, 127 - j] = stencil_weights[a]
    table[left - 1, 128] = stencil_weights[0]
    table[right, 255] = stencil_weights[3]
    return table


def lane_iota(shape):
    return lax.broadcasted_iota(jnp.int32, shape, 1)


def words_wide(words):
    return jnp.concatenate([words, words], axis=0).T


def land_mask(wide, tile):
    lane = lane_iota(wide.shape)
    place = 4 * tile + lax.shift_right_logical(lane, 5)
    word = jnp.take_along_axis(wide, place, axis=1, mode="promise_in_bounds")
    return (word & lax.shift_left(jnp.int32(1), lane & 31)) != 0


def split(x):
    high = x.astype(bf16)
    low = (x - high.astype(f32)).astype(bf16)
    return high, low


def dot(a, b):
    return jnp.dot(a, b, preferred_element_type=f32)


def down_rows(line, count):
    return jnp.broadcast_to(line, (128, 128)).T[0:count]


def rows_down(ref, start, count, *rest):
    index = lambda a: (*rest, pl.ds(start + a, count, stride=2), slice(None))
    outer = ref[index(0)] + ref[index(3)]
    inner = ref[index(1)] + ref[index(2)]
    return stencil_weights[0] * outer + stencil_weights[1] * inner


def on_chip(x):
    return pltpu.with_memory_space_constraint(x, pltpu.VMEM)


def in_hbm(x):
    return pltpu.with_memory_space_constraint(x, pltpu.HBM)


def columns_kernel(
    place_ref, field_ref, words_ref,
    to_left_ref, to_right_ref, near_ref, near_words_ref, cos_ref,
    left_ref, right_ref, sems,
    *, total_rows,
):
    rows, cols = field_ref.shape
    small = [
        pltpu.make_async_copy(words_ref, near_words_ref, sems.at[0]),
        pltpu.make_async_copy(field_ref.at[:, 0:128], left_ref, sems.at[1]),
        pltpu.make_async_copy(field_ref.at[:, cols - 128 : cols], right_ref, sems.at[2]),
    ]
    part = rows // 4
    large = [
        pltpu.make_async_copy(
            field_ref.at[k * part : k * part + part, :],
            near_ref.at[k * part : k * part + part, :],
            sems.at[3 + k],
        )
        for k in range(2)
    ]
    for copy in small + large:
        copy.start()
    line = lax.broadcasted_iota(jnp.int32, (8, 128), 0)
    lane = lane_iota((8, 128))
    around = jnp.where(lane < 16, lane - 16, rows + lane - 16)
    global_rows = place_ref[0] * rows + jnp.where(line < rows // 128, line * 128 + lane, around)
    latitude = ((global_rows.astype(f32) + 0.5) / total_rows - 0.5) * math.pi
    inside = (global_rows >= 0) & (global_rows < total_rows)
    cos_ref[...] = jnp.where(inside, jnp.cos(latitude), 0.0)
    for copy in small:
        copy.wait()
    wide = words_wide(near_words_ref[...])
    left_mask = land_mask(wide, 0)
    right_mask = land_mask(wide, 15)
    lane = lane_iota(left_mask.shape)
    left_land = pltpu.roll(jnp.where(left_mask, 1.0, 0.0), 16, 1)
    right_land = pltpu.roll(jnp.where(right_mask, 1.0, 0.0), 112, 1)
    left_side = jnp.where(lane < 16, jnp.where(left_mask, left_ref[...], 0.0), left_land)
    right_side = jnp.where(lane >= 112, jnp.where(right_mask, right_ref[...], 0.0), right_land)
    both = jnp.where(lane < 64, left_side, right_side).T
    to_left_ref[...] = both[0:32]
    to_right_ref[...] = both[96:128]
    for copy in large:
        copy.wait()


def columns_strips(place, field, words, total_rows):
    rows, cols = field.shape
    return pl.pallas_call(
        functools.partial(columns_kernel, total_rows=total_rows),
        in_specs=[pl.BlockSpec(memory_space=pltpu.SMEM)] + [pl.BlockSpec(memory_space=pl.ANY)] * 2,
        out_specs=[pl.BlockSpec(memory_space=pltpu.VMEM)] * 5,
        out_shape=[
            pltpu.VMEM((32, rows), f32),
            pltpu.VMEM((32, rows), f32),
            pltpu.VMEM((rows // 2, cols), f32),
            pltpu.VMEM(words.shape, words.dtype),
            pltpu.VMEM((8, 128), f32),
        ],
        scratch_shapes=[
            pltpu.VMEM((rows, 128), f32),
            pltpu.VMEM((rows, 128), f32),
            pltpu.SemaphoreType.DMA((5,)),
        ],
        compiler_params=pltpu.CompilerParams(vmem_limit_bytes=vmem_limit),
        name="columns_strips",
    )(place, field, words)


def rows_kernel(
    place_ref, after_ref, upper_ref, lower_ref, words_ref, right_ref, left_ref,
    to_core_ref, to_chip_ref, halo_ref, wide_ref,
):
    del after_ref
    rows = halo_ref.shape[0]
    height = lower_ref.shape[0]
    for part in range(rows // 128):
        cols = slice(part * 128, part * 128 + 128)
        halo_ref[cols, :] = jnp.concatenate(
            [right_ref[:, cols], jnp.zeros((64, 128), f32), left_ref[:, cols]], axis=0
        ).T
    odd = place_ref[0] & 1
    for out_ref, bottom in ((to_core_ref, 1 - odd), (to_chip_ref, odd)):
        first = pl.multiple_of(bottom * (rows - 16), 16)
        wide_ref[...] = words_wide(words_ref[:, pl.ds(pl.multiple_of(bottom * (rows - 128), 128), 128)])
        wide = wide_ref[pl.ds(pl.multiple_of(bottom * 112, 16), 16), :]
        for tile in range(16):
            lanes = slice(tile * 128, tile * 128 + 128)
            mask = land_mask(wide, tile)
            field = jnp.where(
                bottom == 1, lower_ref[height - 16 : height, lanes], upper_ref[0:16, lanes]
            )
            out_ref[0:16, lanes] = jnp.where(mask, field, 0.0)
            out_ref[16:32, lanes] = jnp.where(mask, 1.0, 0.0)
        out_ref[0:16, 2048:2176] = halo_ref[pl.ds(first, 16), :]
        out_ref[16:32, 2048:2176] = jnp.zeros((16, 128), f32)


def rows_strips(place, after, upper, lower, words, from_right, from_left):
    rows, cols = words.shape[1], upper.shape[1]
    return pl.pallas_call(
        rows_kernel,
        in_specs=[pl.BlockSpec(memory_space=pltpu.SMEM)]
        + [pl.BlockSpec(memory_space=pltpu.VMEM)] * 6,
        out_specs=[pl.BlockSpec(memory_space=pltpu.VMEM)] * 3,
        out_shape=[
            pltpu.VMEM((32, cols + 128), f32),
            pltpu.VMEM((32, cols + 128), f32),
            pltpu.VMEM((rows, 128), f32),
        ],
        scratch_shapes=[pltpu.VMEM((128, 128), jnp.int32)],
        compiler_params=pltpu.CompilerParams(vmem_limit_bytes=vmem_limit),
        name="rows_strips",
    )(place, after, upper, lower, words, from_right, from_left)


def side_terms(halo_ref, cos_ref, mixed_ref, side_ref, tall_ref):
    rows = halo_ref.shape[0]
    tall_ref[:, 0:24, :] = jnp.zeros((4, 24, 128), f32)
    tall_ref[:, 24 + rows :, :] = jnp.zeros((4, 24, 128), f32)
    mixed = mixed_ref[...]
    for part in range(rows // 128):
        high, low = split(halo_ref[part * 128 : part * 128 + 128, :])
        across = dot(high, mixed) + dot(low, mixed)
        cos = down_rows(cos_ref[part : part + 1, :], 128)
        for k in range(4):
            tall_ref[k, 24 + part * 128 : 152 + part * 128, :] = (
                across[:, k * 128 : k * 128 + 128] * cos
            )
    for k in range(4):
        side_ref[k] = rows_down(tall_ref, 7, side_ref.shape[1], k)


def lower_kernel(
    halo_ref, mixed_ref, field_ref, words_ref, cos_ref, band_ref,
    num_ref, den_ref, side_ref, *scratch, skip,
):
    @pl.when(pl.program_id(0) == 0)
    def _():
        side_terms(halo_ref, cos_ref, mixed_ref, side_ref, scratch[-1])

    upper_kernel(field_ref, words_ref, cos_ref, band_ref, num_ref, den_ref, *scratch[:-1], skip=skip)


def first_kernel(
    whole_ref, field_ref, words_ref, cos_ref, band_ref,
    num_ref, den_ref, lower_ref, *scratch, skip,
):
    height = lower_ref.shape[0]
    copy = pltpu.make_async_copy(
        whole_ref.at[height : 2 * height, :], lower_ref, scratch[-1].at[0]
    )

    @pl.when(pl.program_id(0) == 0)
    def _():
        copy.start()

    upper_kernel(field_ref, words_ref, cos_ref, band_ref, num_ref, den_ref, *scratch[:-1], skip=skip)

    @pl.when(pl.program_id(0) == pl.num_programs(0) - 1)
    def _():
        copy.wait()


def upper_kernel(
    field_ref, words_ref, cos_ref, band_ref, num_ref, den_ref,
    product_ref, cover_ref, main_ref, edge_ref, sheet_ref,
    *, skip,
):
    step = pl.program_id(0)
    blocks = pl.num_programs(0) - 1
    height = field_ref.shape[0]

    @pl.when(step == 0)
    def _():
        sheet_ref[:, :, 0:24, :] = jnp.zeros((2, 9, 24, 128), f32)
        sheet_ref[:, :, 24 + 2 * height :, :] = jnp.zeros(
            (2, 9, sheet_ref.shape[2] - 24 - 2 * height, 128), f32
        )

    @pl.when(step < blocks)
    def _():
        wide = words_wide(words_ref[...])
        for tile in range(8):
            part = slice(tile * height, tile * height + height)
            for half in range(2):
                lanes = slice(tile * 256 + half * 128, tile * 256 + half * 128 + 128)
                mask = land_mask(wide, 2 * tile + half)
                high, low = split(jnp.where(mask, field_ref[:, lanes], 0.0))
                product_ref[part, half * 128 : half * 128 + 128] = high
                product_ref[part, 256 + half * 128 : 384 + half * 128] = low
                cover_ref[part, half * 128 : half * 128 + 128] = jnp.where(mask, 1.0, 0.0).astype(
                    bf16
                )
        cos = down_rows(cos_ref[pl.ds(skip + step, 1), :], 128)
        low_half = lane_iota((height, 128)) < 64
        start = pl.multiple_of(24 + step * height, 8)
        for which, (lhs_ref, depth) in enumerate(((product_ref, 512), (cover_ref, 256))):
            across = dot(lhs_ref[...], band_ref[0:depth, :])
            main_ref[...] = across[:, 0:128]
            edge_ref[...] = across[:, 128:256]
            zero = jnp.zeros((height, 128), f32)
            for t in range(9):
                get = lambda ref, k: ref[k * height : k * height + height, :]
                main = get(main_ref, t) if t < 8 else zero
                before = get(edge_ref, t - 1) if t > 0 else zero
                after = get(edge_ref, (t + 1) % 9) if t != 7 else zero
                sheet_ref[which, t, pl.ds(start, height), :] = (
                    main + jnp.where(low_half, before, after)
                ) * cos

    def down(count):
        first = 7 + step * height
        place = pl.multiple_of(step * (height // 2), 8)
        for which, out_ref in ((0, num_ref), (1, den_ref)):
            for t in range(9):
                out_ref[pl.ds(place, count), t * 128 : t * 128 + 128] = rows_down(
                    sheet_ref, first, count, which, t
                )

    @pl.when(step < blocks)
    def _():
        down(height // 2)

    @pl.when(step == blocks)
    def _():
        down(16)


def own_level(field, words, cosines, band, part, *beside):
    height = 128
    blocks = field.shape[0] // height
    rows, cols = 2 * field.shape[0], field.shape[1]
    skip = part * blocks
    vmem = pl.BlockSpec(memory_space=pltpu.VMEM)
    half = pltpu.VMEM((blocks * height // 2 + 16, cols // 2 + 128), f32)
    if part == 0:
        kernel, given = first_kernel, [pl.BlockSpec(memory_space=pl.ANY)]
        more, scratch = pltpu.VMEM(field.shape, f32), pltpu.SemaphoreType.DMA((1,))
    else:
        kernel, given = lower_kernel, [vmem, vmem]
        more, scratch = pltpu.VMEM((4, rows // 2 + 16, 128), f32), pltpu.VMEM((4, rows + 48, 128), f32)
    at = lambda b: jnp.minimum(b, blocks - 1)
    return pl.pallas_call(
        functools.partial(kernel, skip=skip),
        grid=(blocks + 1,),
        in_specs=given
        + [
            pl.BlockSpec((height, cols), lambda b: (at(b), 0)),
            pl.BlockSpec((64, height), lambda b: (0, skip + at(b))),
            pl.BlockSpec((8, 128), lambda b: (0, 0)),
            pl.BlockSpec((512, 256), lambda b: (0, 0)),
        ],
        out_specs=[vmem] * 3,
        out_shape=[half, half, more],
        scratch_shapes=[
            pltpu.VMEM((8 * height, 512), bf16),
            pltpu.VMEM((8 * height, 256), bf16),
            pltpu.VMEM((8 * height, 128), f32),
            pltpu.VMEM((8 * height, 128), f32),
            pltpu.VMEM((2, 9, 24 + (blocks + 1) * height, 128), f32),
            scratch,
        ],
        compiler_params=pltpu.CompilerParams(vmem_limit_bytes=vmem_limit),
        name="own_level",
    )(*beside, field, words, cosines, band)


def fold(x):
    return x.reshape(x.shape[0] // 8, 8, 128)


def levels_kernel(
    place_ref, num_a_ref, den_a_ref, num_b_ref, den_b_ref, side_ref, core_ref, chip_ref, cos_ref,
    band_ref, band_halo_ref, band_mixed_ref,
    one_ref, two_ref, three_ref, four_ref, stats_ref,
    p1_ref, c1_ref, p2_ref, c2_ref, p3_ref, c3_ref, tall_ref, strip_ref, value_ref,
    *, last_place,
):
    count = side_ref.shape[1]
    rows = 2 * (count - 16)
    band = band_ref[...]
    mixed = band_mixed_ref[...]
    odd = (place_ref[0] & 1) == 1
    tall_ref[:, 0:8, :] = jnp.zeros((4, 8, 128), f32)

    def pick(before, after):
        shape = before.shape
        return jnp.where(lane_iota(shape) < 64, before, after)

    last = 7 * 128
    add_p, edge_p, add_c, edge_c = (side_ref[k] for k in range(4))
    mid = rows // 4
    for a_ref, b_ref, out_ref, add, edge in (
        (num_a_ref, num_b_ref, p1_ref, add_p, edge_p),
        (den_a_ref, den_b_ref, c1_ref, add_c, edge_c),
    ):
        lower = lane_iota(edge.shape) < 64
        out_ref[0:mid, :] = a_ref[0:mid, :]
        out_ref[mid : mid + 16, :] = a_ref[mid : mid + 16, :] + b_ref[0:16, :]
        out_ref[mid + 16 : count, :] = b_ref[16 : mid + 16, :]
        out_ref[:, 0:128] = out_ref[:, 0:128] + jnp.where(lower, edge, 0.0)
        out_ref[:, last : last + 128] = out_ref[:, last : last + 128] + jnp.where(
            lower, 0.0, edge
        )
        out_ref[:, 1024:1152] = out_ref[:, 1024:1152] + add

    strip_ref[...] = jnp.zeros(strip_ref.shape, f32)
    ends_cos = down_rows(cos_ref[4:5, :], 32)
    for side, (cos, first) in enumerate(((ends_cos[0:16], 8), (ends_cos[16:32], 24))):
        of_core = odd if side == 0 else jnp.logical_not(odd)
        strip = jnp.where(of_core, core_ref[...], chip_ref[...])
        lhs = []
        for t in range(8):
            high, low = split(strip[0:16, t * 256 : t * 256 + 256])
            lhs += [high, low, strip[16:32, t * 256 : t * 256 + 256].astype(bf16)]
        out = dot(jnp.concatenate(lhs, axis=0), band)
        high, low = split(strip[0:16, 2048:2176])
        corner = dot(high, mixed) + dot(low, mixed)
        for which in range(2):
            parts = []
            for t in range(8):
                base = t * 48
                if which == 0:
                    parts.append(out[base : base + 16] + out[base + 16 : base + 32])
                else:
                    parts.append(out[base + 32 : base + 48])
            parts.append(corner[:, which * 256 : which * 256 + 256])
            for t in range(9):
                edges = pick(parts[(t - 1) % 9][:, 128:256], parts[(t + 1) % 9][:, 128:256])
                strip_ref[side, which, t, first : first + 16, :] = (
                    parts[t][:, 0:128] + edges
                ) * cos
        where = slice(0, 16) if side == 0 else slice(rows // 2, rows // 2 + 16)
        for which, out_ref in ((0, p1_ref), (1, c1_ref)):
            for t in range(9):
                lanes = slice(t * 128, t * 128 + 128)
                extra = rows_down(strip_ref, 7, 16, side, which, t)
                out_ref[where, lanes] = out_ref[where, lanes] + extra

    at_first = (place_ref[0] == 0).astype(jnp.int32)
    at_last = (place_ref[0] == last_place).astype(jnp.int32)
    sums = []

    def finish(num, den, halo, own):
        value = num / jnp.maximum(den, floor_value)
        row = lax.broadcasted_iota(jnp.int32, num.shape, 0)
        inside = (row >= halo * at_first) & (row < own + halo + (1 - at_last) * 4096)
        cover = jnp.where(inside, den, 0.0)
        return value, cover * value, cover

    level_one_sums = None
    for t in range(9):
        lanes = slice(t * 128, t * 128 + 128)
        value, product, cover = finish(p1_ref[:, lanes], c1_ref[:, lanes], 8, rows // 2)
        p1_ref[:, lanes] = product
        c1_ref[:, lanes] = cover
        if t < 8:
            own = slice(8, 8 + rows // 2)
            one_ref[:, lanes] = value[own]
            new = (
                jnp.sum(fold(product[own]), 0),
                jnp.sum(fold(cover[own]), 0),
                jnp.max(fold(value[own]), 0),
            )
            if level_one_sums is None:
                level_one_sums = new
            else:
                old = level_one_sums
                level_one_sums = (
                    old[0] + new[0], old[1] + new[1], jnp.maximum(old[2], new[2])
                )
    sums.append(level_one_sums)

    def next_level(p_ref, c_ref, tiles, in_rows, out_rows, halo, own_rows, out_ref, p_out, c_out):
        total = None
        nums = []
        dens = []
        for ref, dest in ((p_ref, nums), (c_ref, dens)):
            blocks = []
            for t in range(tiles):
                high, low = split(ref[:, t * 256 : t * 256 + 256])
                blocks.append(dot(high, band) + dot(low, band))
            high, low = split(ref[:, tiles * 256 : tiles * 256 + 128])
            ring = band_halo_ref[...]
            blocks.append(dot(high, ring) + dot(low, ring))
            count = tiles + 1
            for t in range(count):
                across = blocks[t][:, 0:128] + pick(
                    blocks[(t - 1) % count][:, 128:256], blocks[(t + 1) % count][:, 128:256]
                )
                slot = t % 4
                tall_ref[slot, 8 : 8 + in_rows, :] = across
                tall_ref[slot, 8 + in_rows : 2 * out_rows + 16, :] = jnp.zeros(
                    (2 * out_rows + 8 - in_rows, 128), f32
                )
                dest.append(rows_down(tall_ref, 7, out_rows, slot))
        for t in range(tiles + 1):
            value, product, cover = finish(nums[t], dens[t], halo, own_rows)
            if p_out is not None:
                p_out[:, t * 128 : t * 128 + 128] = product
                c_out[:, t * 128 : t * 128 + 128] = cover
            if t < tiles:
                own = slice(halo, halo + own_rows)
                value_ref[0, 0:out_rows, :] = value
                value_ref[1, 0:out_rows, :] = product
                value_ref[2, 0:out_rows, :] = cover
                v, p, c = (value_ref[k, own, :] for k in range(3))
                out_ref[:, t * 128 : t * 128 + 128] = v
                new = (jnp.sum(fold(p), 0), jnp.sum(fold(c), 0), jnp.max(fold(v), 0))
                total = (
                    new
                    if total is None
                    else (total[0] + new[0], total[1] + new[1], jnp.maximum(total[2], new[2]))
                )
        sums.append(total)

    next_level(p1_ref, c1_ref, 4, 272, 136, 4, 128, two_ref, p2_ref, c2_ref)
    next_level(p2_ref, c2_ref, 2, 136, 72, 2, 64, three_ref, p3_ref, c3_ref)
    next_level(p3_ref, c3_ref, 1, 72, 40, 1, 32, four_ref, None, None)

    lane = lane_iota((1, 128))
    row = jnp.zeros((1, 128), f32)
    for level in range(4):
        for kind in range(3):
            part = sums[level][kind]
            one = (jnp.max if kind == 2 else jnp.sum)(part, axis=0, keepdims=True)
            one = (jnp.max if kind == 2 else jnp.sum)(one, axis=1, keepdims=True)
            row = jnp.where(lane == kind * 4 + level, one, row)
    stats_ref[...] = jnp.broadcast_to(row, stats_ref.shape)


def all_levels(place, last_place, chips, owns, by_core, by_chip, cosines, tables, rows, cols):
    vmem = pl.BlockSpec(memory_space=pltpu.VMEM)
    shapes = [(rows >> k, cols >> k) for k in (1, 2, 3, 4)]
    outs = [pltpu.VMEM(shape, f32) for shape in shapes]
    half = rows // 2 + 16
    return pl.pallas_call(
        functools.partial(levels_kernel, last_place=last_place),
        in_specs=[pl.BlockSpec(memory_space=pltpu.SMEM)] + [vmem] * 11,
        out_specs=[vmem] * 5,
        out_shape=outs + [pltpu.VMEM((chips, 128), f32)],
        scratch_shapes=[
            pltpu.VMEM((half, cols // 2 + 128), f32),
            pltpu.VMEM((half, cols // 2 + 128), f32),
            pltpu.VMEM((136, cols // 4 + 128), f32),
            pltpu.VMEM((136, cols // 4 + 128), f32),
            pltpu.VMEM((72, cols // 8 + 128), f32),
            pltpu.VMEM((72, cols // 8 + 128), f32),
            pltpu.VMEM((4, rows + 48, 128), f32),
            pltpu.VMEM((2, 2, 9, 48, 128), f32),
            pltpu.VMEM((3, 136, 128), f32),
        ],
        compiler_params=pltpu.CompilerParams(vmem_limit_bytes=vmem_limit),
        name="all_levels",
    )(place, *owns, by_core, by_chip, cosines, *tables)


def emit_kernel(after_ref, *refs):
    del after_ref
    *refs, sems = refs
    copies = [
        pltpu.make_async_copy(refs[k], refs[k + 4], sems.at[k]) for k in range(4)
    ]
    for copy in copies:
        copy.start()
    for copy in copies:
        copy.wait()


def emit(after, levels):
    return pl.pallas_call(
        emit_kernel,
        in_specs=[pl.BlockSpec(memory_space=pltpu.VMEM)] * 5,
        out_specs=[pl.BlockSpec(memory_space=pl.ANY)] * 4,
        out_shape=[jax.ShapeDtypeStruct(level.shape, f32) for level in levels],
        scratch_shapes=[pltpu.SemaphoreType.DMA((4,))],
        compiler_params=pltpu.CompilerParams(vmem_limit_bytes=vmem_limit),
        name="emit",
    )(after, *[on_chip(level) for level in levels])


def per_device(surface_field, land_words):
    rows, cols = surface_field.shape
    row_devices = lax.axis_size(ROWS)
    col_devices = lax.axis_size(COLS)
    total_rows = rows * row_devices
    position = lax.axis_index(ROWS)

    band = jnp.asarray(band_main(), bf16)
    ring = jnp.asarray(band_halo(64, 0, 128), bf16)
    mixed = jnp.asarray(
        np.concatenate([band_halo(16, 0, 128), band_halo(16, 16, 112)], axis=1), bf16
    )

    place = jnp.reshape(position, (1,))
    words = land_words.T

    east = [(i, (i + 1) % col_devices) for i in range(col_devices)]
    west = [(target, source) for source, target in east]

    to_left, to_right, near, near_words, cosines = columns_strips(
        place, in_hbm(surface_field), in_hbm(words), total_rows
    )
    near, near_words, cosines = on_chip(near), on_chip(near_words), on_chip(cosines)
    from_right = lax.ppermute(to_left, COLS, west)
    from_left = lax.ppermute(to_right, COLS, east)
    twice = jnp.concatenate([band, band], axis=0)
    *upper, lower_near = own_level(near, near_words, cosines, twice, 0, in_hbm(surface_field))
    lower_near = on_chip(lower_near)
    to_core, to_chip, halo = rows_strips(
        place, on_chip(upper[0]), near, lower_near, near_words, on_chip(from_right), on_chip(from_left)
    )
    by_core = lax.ppermute(to_core, ROWS, [(i, i ^ 1) for i in range(row_devices)])
    by_chip = lax.ppermute(to_chip, ROWS, [(i, ((i - 1) ^ 1) + 1) for i in range(1, row_devices - 1)])
    lower = own_level(lower_near, near_words, cosines, twice, 1, on_chip(halo), mixed)
    chips = lax.axis_size(CHIPS)
    *levels, stats = all_levels(
        place, row_devices - 1, chips, [on_chip(x) for x in (*upper, *lower)],
        on_chip(by_core), on_chip(by_chip), cosines, (band, ring, mixed), rows, cols,
    )

    is_sum = jnp.arange(128) < 8
    every = lax.all_to_all(stats, CHIPS, 0, 0, tiled=True)
    stats = jnp.where(is_sum, jnp.sum(every, axis=0), jnp.max(every, axis=0))
    other = lax.ppermute(stats, CORE, [(0, 1), (1, 0)])
    one, two, three, four = emit(on_chip(stats), levels)
    sums = stats[0:8] + other[0:8]
    maxima = jnp.maximum(stats[8:12], other[8:12])
    means = sums[0:4] / (sums[4:8] + mean_eps)
    return (one, two, three, four, means, maxima)


def solution(mesh):
    finer = Mesh(
        mesh.devices.reshape(2, 4, 2, 2, 4), ("rows_0", "rows_1", "rows_2", "cols_0", "cols_1")
    )
    in_specs = (P(ROWS, COLS), P(ROWS, COLS))
    out_specs = (P(ROWS, COLS), P(ROWS, COLS), P(ROWS, COLS), P(ROWS, COLS), P(), P())
    return jax.shard_map(
        per_device, mesh=finer, in_specs=in_specs, out_specs=out_specs, check_vma=False
    )
```

```python
import functools
import math

import jax
import jax.numpy as jnp
import numpy as np
from jax import lax
from jax.experimental import pallas as pl
from jax.experimental.pallas import tpu as pltpu
from jax.sharding import Mesh
from jax.sharding import PartitionSpec as P

ROWS = ("rows_0", "rows_1", "rows_2")
COLS = ("cols_0", "cols_1")
CHIPS = ("rows_0", "rows_1", "cols_0", "cols_1")
CORE = "rows_2"


stencil_weights = (0.125, 0.375, 0.375, 0.125)
floor_value = 0.05
mean_eps = 1e-06

vmem_limit = 20 * 1024 * 1024

f32 = jnp.float32
bf16 = jnp.bfloat16


def band_main():
    table = np.zeros((256, 256), np.float32)
    for j in range(128):
        for a in range(4):
            k = 2 * j - 1 + a
            if 0 <= k < 256:
                table[k, j] = stencil_weights[a]
    table[255, 128] = stencil_weights[0]
    table[0, 255] = stencil_weights[3]
    return table


def band_halo(width, right, left):
    table = np.zeros((128, 256), np.float32)
    for j in range(width // 2):
        for a in range(4):
            k = 2 * j - 1 + a
            if 0 <= k < width:
                table[right + k, j] = stencil_weights[a]
        for a in range(4):
            k = -3 - 2 * j + a
            if -width <= k < 0:
                table[left + k, 127 - j] = stencil_weights[a]
    table[left - 1, 128] = stencil_weights[0]
    table[right, 255] = stencil_weights[3]
    return table


def lane_iota(shape):
    return lax.broadcasted_iota(jnp.int32, shape, 1)


def words_wide(words):
    return jnp.concatenate([words, words], axis=0).T


def land_mask(wide, tile):
    lane = lane_iota(wide.shape)
    place = 4 * tile + lax.shift_right_logical(lane, 5)
    word = jnp.take_along_axis(wide, place, axis=1, mode="promise_in_bounds")
    return (word & lax.shift_left(jnp.int32(1), lane & 31)) != 0


def split(x):
    high = x.astype(bf16)
    low = (x - high.astype(f32)).astype(bf16)
    return high, low


def dot(a, b):
    return jnp.dot(a, b, preferred_element_type=f32)


def down_rows(line, count):
    return jnp.broadcast_to(line, (128, 128)).T[0:count]


def rows_down(ref, start, count, *rest):
    index = lambda a: (*rest, pl.ds(start + a, count, stride=2), slice(None))
    outer = ref[index(0)] + ref[index(3)]
    inner = ref[index(1)] + ref[index(2)]
    return stencil_weights[0] * outer + stencil_weights[1] * inner


def on_chip(x):
    return pltpu.with_memory_space_constraint(x, pltpu.VMEM)


def in_hbm(x):
    return pltpu.with_memory_space_constraint(x, pltpu.HBM)


def columns_kernel(
    place_ref, field_ref, words_ref,
    to_left_ref, to_right_ref, near_ref, near_words_ref, cos_ref,
    left_ref, right_ref, sems,
    *, total_rows,
):
    rows, cols = field_ref.shape
    small = [
        pltpu.make_async_copy(words_ref, near_words_ref, sems.at[0]),
        pltpu.make_async_copy(field_ref.at[:, 0:128], left_ref, sems.at[1]),
        pltpu.make_async_copy(field_ref.at[:, cols - 128 : cols], right_ref, sems.at[2]),
    ]
    part = rows // 4
    large = [
        pltpu.make_async_copy(
            field_ref.at[k * part : k * part + part, :],
            near_ref.at[k * part : k * part + part, :],
            sems.at[3 + k],
        )
        for k in range(2)
    ]
    for copy in small + large:
        copy.start()
    line = lax.broadcasted_iota(jnp.int32, (8, 128), 0)
    global_rows = place_ref[0] * rows + line * 128 + lane_iota((8, 128))
    latitude = ((global_rows.astype(f32) + 0.5) / total_rows - 0.5) * math.pi
    cos_ref[...] = jnp.cos(latitude)
    for copy in small:
        copy.wait()
    wide = words_wide(near_words_ref[...])
    left_mask = land_mask(wide, 0)
    right_mask = land_mask(wide, 15)
    lane = lane_iota(left_mask.shape)
    left_land = pltpu.roll(jnp.where(left_mask, 1.0, 0.0), 16, 1)
    right_land = pltpu.roll(jnp.where(right_mask, 1.0, 0.0), 112, 1)
    left_side = jnp.where(lane < 16, jnp.where(left_mask, left_ref[...], 0.0), left_land)
    right_side = jnp.where(lane >= 112, jnp.where(right_mask, right_ref[...], 0.0), right_land)
    both = jnp.where(lane < 64, left_side, right_side).T
    to_left_ref[...] = both[0:32]
    to_right_ref[...] = both[96:128]
    for copy in large:
        copy.wait()


def columns_strips(place, field, words, total_rows):
    rows, cols = field.shape
    return pl.pallas_call(
        functools.partial(columns_kernel, total_rows=total_rows),
        in_specs=[pl.BlockSpec(memory_space=pltpu.SMEM)] + [pl.BlockSpec(memory_space=pl.ANY)] * 2,
        out_specs=[pl.BlockSpec(memory_space=pltpu.VMEM)] * 5,
        out_shape=[
            pltpu.VMEM((32, rows), f32),
            pltpu.VMEM((32, rows), f32),
            pltpu.VMEM((rows // 2, cols), f32),
            pltpu.VMEM(words.shape, words.dtype),
            pltpu.VMEM((8, 128), f32),
        ],
        scratch_shapes=[
            pltpu.VMEM((rows, 128), f32),
            pltpu.VMEM((rows, 128), f32),
            pltpu.SemaphoreType.DMA((5,)),
        ],
        compiler_params=pltpu.CompilerParams(vmem_limit_bytes=vmem_limit),
        name="columns_strips",
    )(place, field, words)


def rows_kernel(
    place_ref, after_ref, upper_ref, lower_ref, words_ref, right_ref, left_ref,
    cos_ref, band_ref, mixed_ref,
    to_core_ref, to_chip_ref, halo_ref, wide_ref, lhs_ref, corner_ref,
):
    del after_ref
    rows = halo_ref.shape[0]
    height = lower_ref.shape[0]
    for part in range(rows // 128):
        cols = slice(part * 128, part * 128 + 128)
        halo_ref[cols, :] = jnp.concatenate(
            [right_ref[:, cols], jnp.zeros((64, 128), f32), left_ref[:, cols]], axis=0
        ).T
    odd = place_ref[0] & 1
    cos_top = down_rows(cos_ref[0:1, :], 16)
    cos_bottom = down_rows(cos_ref[3:4, :], 128)[112:128]
    sides = ((to_core_ref, 1 - odd), (to_chip_ref, odd))
    for side, (_, bottom) in enumerate(sides):
        first = pl.multiple_of(bottom * (rows - 16), 16)
        wide_ref[...] = words_wide(words_ref[:, pl.ds(pl.multiple_of(bottom * (rows - 128), 128), 128)])
        wide = wide_ref[pl.ds(pl.multiple_of(bottom * 112, 16), 16), :]
        for tile in range(16):
            lanes = slice(tile * 128, tile * 128 + 128)
            half = slice(tile % 2 * 128, tile % 2 * 128 + 128)
            mask = land_mask(wide, tile)
            field = jnp.where(
                bottom == 1, lower_ref[height - 16 : height, lanes], upper_ref[0:16, lanes]
            )
            high, low = split(jnp.where(mask, field, 0.0))
            land = jnp.where(mask, 1.0, 0.0).astype(bf16)
            base = side * 384 + tile // 2 * 48
            for k, value in enumerate((high, low, land)):
                lhs_ref[base + k * 16 : base + k * 16 + 16, half] = value
        high, low = split(halo_ref[pl.ds(first, 16), :])
        corner_ref[side * 32 : side * 32 + 16, :] = high
        corner_ref[side * 32 + 16 : side * 32 + 32, :] = low
    across = dot(lhs_ref[...], band_ref[...])
    corners = dot(corner_ref[...], mixed_ref[...])
    low_half = lane_iota((16, 128)) < 64
    for side, (out_ref, bottom) in enumerate(sides):
        cos = jnp.where(bottom == 1, cos_bottom, cos_top)
        corner = corners[side * 32 : side * 32 + 16] + corners[side * 32 + 16 : side * 32 + 32]
        for which in range(2):
            parts = []
            for t in range(8):
                base = side * 384 + t * 48
                if which == 0:
                    parts.append(across[base : base + 16] + across[base + 16 : base + 32])
                else:
                    parts.append(across[base + 32 : base + 48])
            parts.append(corner[:, which * 256 : which * 256 + 256])
            for t in range(9):
                edges = jnp.where(
                    low_half, parts[(t - 1) % 9][:, 128:256], parts[(t + 1) % 9][:, 128:256]
                )
                out_ref[which * 16 : which * 16 + 16, t * 128 : t * 128 + 128] = (
                    parts[t][:, 0:128] + edges
                ) * cos


def rows_strips(place, after, upper, lower, words, from_right, from_left, cosines, tables):
    rows, cols = words.shape[1], upper.shape[1]
    return pl.pallas_call(
        rows_kernel,
        in_specs=[pl.BlockSpec(memory_space=pltpu.SMEM)]
        + [pl.BlockSpec(memory_space=pltpu.VMEM)] * 9,
        out_specs=[pl.BlockSpec(memory_space=pltpu.VMEM)] * 3,
        out_shape=[
            pltpu.VMEM((32, cols // 2 + 128), f32),
            pltpu.VMEM((32, cols // 2 + 128), f32),
            pltpu.VMEM((rows, 128), f32),
        ],
        scratch_shapes=[
            pltpu.VMEM((128, 128), jnp.int32),
            pltpu.VMEM((768, 256), bf16),
            pltpu.VMEM((64, 128), bf16),
        ],
        compiler_params=pltpu.CompilerParams(vmem_limit_bytes=vmem_limit),
        name="rows_strips",
    )(place, after, upper, lower, words, from_right, from_left, cosines, *tables)


def side_terms(halo_ref, cos_ref, mixed_ref, side_ref, tall_ref):
    rows = halo_ref.shape[0]
    tall_ref[:, 0:24, :] = jnp.zeros((4, 24, 128), f32)
    tall_ref[:, 24 + rows :, :] = jnp.zeros((4, 24, 128), f32)
    mixed = mixed_ref[...]
    for part in range(rows // 128):
        high, low = split(halo_ref[part * 128 : part * 128 + 128, :])
        across = dot(high, mixed) + dot(low, mixed)
        cos = down_rows(cos_ref[part : part + 1, :], 128)
        for k in range(4):
            tall_ref[k, 24 + part * 128 : 152 + part * 128, :] = (
                across[:, k * 128 : k * 128 + 128] * cos
            )
    for k in range(4):
        side_ref[k] = rows_down(tall_ref, 7, side_ref.shape[1], k)


def lower_kernel(
    halo_ref, mixed_ref, field_ref, words_ref, cos_ref, band_ref,
    num_ref, den_ref, side_ref, *scratch, skip,
):
    @pl.when(pl.program_id(0) == 0)
    def _():
        side_terms(halo_ref, cos_ref, mixed_ref, side_ref, scratch[-1])

    upper_kernel(field_ref, words_ref, cos_ref, band_ref, num_ref, den_ref, *scratch[:-1], skip=skip)


def first_kernel(
    whole_ref, field_ref, words_ref, cos_ref, band_ref,
    num_ref, den_ref, lower_ref, *scratch, skip,
):
    height = lower_ref.shape[0]
    copy = pltpu.make_async_copy(
        whole_ref.at[height : 2 * height, :], lower_ref, scratch[-1].at[0]
    )

    @pl.when(pl.program_id(0) == 0)
    def _():
        copy.start()

    upper_kernel(field_ref, words_ref, cos_ref, band_ref, num_ref, den_ref, *scratch[:-1], skip=skip)

    @pl.when(pl.program_id(0) == pl.num_programs(0) - 1)
    def _():
        copy.wait()


def upper_kernel(
    field_ref, words_ref, cos_ref, band_ref, num_ref, den_ref,
    product_ref, cover_ref, main_ref, edge_ref, sheet_ref,
    *, skip,
):
    step = pl.program_id(0)
    blocks = pl.num_programs(0) - 1
    height = field_ref.shape[0]

    @pl.when(step == 0)
    def _():
        sheet_ref[:, :, 0:24, :] = jnp.zeros((2, 9, 24, 128), f32)
        sheet_ref[:, :, 24 + 2 * height :, :] = jnp.zeros(
            (2, 9, sheet_ref.shape[2] - 24 - 2 * height, 128), f32
        )

    @pl.when(step < blocks)
    def _():
        wide = words_wide(words_ref[...])
        for tile in range(8):
            part = slice(tile * height, tile * height + height)
            for half in range(2):
                lanes = slice(tile * 256 + half * 128, tile * 256 + half * 128 + 128)
                mask = land_mask(wide, 2 * tile + half)
                high, low = split(jnp.where(mask, field_ref[:, lanes], 0.0))
                product_ref[part, half * 128 : half * 128 + 128] = high
                product_ref[part, 256 + half * 128 : 384 + half * 128] = low
                cover_ref[part, half * 128 : half * 128 + 128] = jnp.where(mask, 1.0, 0.0).astype(
                    bf16
                )
        cos = down_rows(cos_ref[pl.ds(skip + step, 1), :], 128)
        low_half = lane_iota((height, 128)) < 64
        start = pl.multiple_of(24 + step * height, 8)
        for which, (lhs_ref, depth) in enumerate(((product_ref, 512), (cover_ref, 256))):
            across = dot(lhs_ref[...], band_ref[0:depth, :])
            main_ref[...] = across[:, 0:128]
            edge_ref[...] = across[:, 128:256]
            zero = jnp.zeros((height, 128), f32)
            for t in range(9):
                get = lambda ref, k: ref[k * height : k * height + height, :]
                main = get(main_ref, t) if t < 8 else zero
                before = get(edge_ref, t - 1) if t > 0 else zero
                after = get(edge_ref, (t + 1) % 9) if t != 7 else zero
                sheet_ref[which, t, pl.ds(start, height), :] = (
                    main + jnp.where(low_half, before, after)
                ) * cos

    def down(count):
        first = 7 + step * height
        place = pl.multiple_of(step * (height // 2), 8)
        for which, out_ref in ((0, num_ref), (1, den_ref)):
            for t in range(9):
                out_ref[pl.ds(place, count), t * 128 : t * 128 + 128] = rows_down(
                    sheet_ref, first, count, which, t
                )

    @pl.when(step < blocks)
    def _():
        down(height // 2)

    @pl.when(step == blocks)
    def _():
        down(16)


def own_level(field, words, cosines, band, part, *beside):
    height = 128
    blocks = field.shape[0] // height
    rows, cols = 2 * field.shape[0], field.shape[1]
    skip = part * blocks
    vmem = pl.BlockSpec(memory_space=pltpu.VMEM)
    half = pltpu.VMEM((blocks * height // 2 + 16, cols // 2 + 128), f32)
    if part == 0:
        kernel, given = first_kernel, [pl.BlockSpec(memory_space=pl.ANY)]
        more, scratch = pltpu.VMEM(field.shape, f32), pltpu.SemaphoreType.DMA((1,))
    else:
        kernel, given = lower_kernel, [vmem, vmem]
        more, scratch = pltpu.VMEM((4, rows // 2 + 16, 128), f32), pltpu.VMEM((4, rows + 48, 128), f32)
    at = lambda b: jnp.minimum(b, blocks - 1)
    return pl.pallas_call(
        functools.partial(kernel, skip=skip),
        grid=(blocks + 1,),
        in_specs=given
        + [
            pl.BlockSpec((height, cols), lambda b: (at(b), 0)),
            pl.BlockSpec((64, height), lambda b: (0, skip + at(b))),
            pl.BlockSpec((8, 128), lambda b: (0, 0)),
            pl.BlockSpec((512, 256), lambda b: (0, 0)),
        ],
        out_specs=[vmem] * 3,
        out_shape=[half, half, more],
        scratch_shapes=[
            pltpu.VMEM((8 * height, 512), bf16),
            pltpu.VMEM((8 * height, 256), bf16),
            pltpu.VMEM((8 * height, 128), f32),
            pltpu.VMEM((8 * height, 128), f32),
            pltpu.VMEM((2, 9, 24 + (blocks + 1) * height, 128), f32),
            scratch,
        ],
        compiler_params=pltpu.CompilerParams(vmem_limit_bytes=vmem_limit),
        name="own_level",
    )(*beside, field, words, cosines, band)


def fold(x):
    return x.reshape(x.shape[0] // 8, 8, 128)


def levels_kernel(
    place_ref, num_a_ref, den_a_ref, num_b_ref, den_b_ref, side_ref, core_ref, chip_ref,
    band_ref, band_halo_ref,
    one_ref, two_ref, three_ref, four_ref, stats_ref,
    p1_ref, c1_ref, p2_ref, c2_ref, p3_ref, c3_ref, tall_ref, strip_ref, value_ref,
    *, last_place,
):
    count = side_ref.shape[1]
    rows = 2 * (count - 16)
    band = band_ref[...]
    odd = (place_ref[0] & 1) == 1
    tall_ref[:, 0:8, :] = jnp.zeros((4, 8, 128), f32)

    def pick(before, after):
        shape = before.shape
        return jnp.where(lane_iota(shape) < 64, before, after)

    last = 7 * 128
    add_p, edge_p, add_c, edge_c = (side_ref[k] for k in range(4))
    mid = rows // 4
    for a_ref, b_ref, out_ref, add, edge in (
        (num_a_ref, num_b_ref, p1_ref, add_p, edge_p),
        (den_a_ref, den_b_ref, c1_ref, add_c, edge_c),
    ):
        lower = lane_iota(edge.shape) < 64
        out_ref[0:mid, :] = a_ref[0:mid, :]
        out_ref[mid : mid + 16, :] = a_ref[mid : mid + 16, :] + b_ref[0:16, :]
        out_ref[mid + 16 : count, :] = b_ref[16 : mid + 16, :]
        out_ref[:, 0:128] = out_ref[:, 0:128] + jnp.where(lower, edge, 0.0)
        out_ref[:, last : last + 128] = out_ref[:, last : last + 128] + jnp.where(
            lower, 0.0, edge
        )
        out_ref[:, 1024:1152] = out_ref[:, 1024:1152] + add

    strip_ref[...] = jnp.zeros(strip_ref.shape, f32)
    for side, first in ((0, 8), (1, 24)):
        of_core = odd if side == 0 else jnp.logical_not(odd)
        strip = jnp.where(of_core, core_ref[...], chip_ref[...])
        for which in range(2):
            for t in range(9):
                strip_ref[side, which, t, first : first + 16, :] = strip[
                    which * 16 : which * 16 + 16, t * 128 : t * 128 + 128
                ]
        where = slice(0, 16) if side == 0 else slice(rows // 2, rows // 2 + 16)
        for which, out_ref in ((0, p1_ref), (1, c1_ref)):
            for t in range(9):
                lanes = slice(t * 128, t * 128 + 128)
                extra = rows_down(strip_ref, 7, 16, side, which, t)
                out_ref[where, lanes] = out_ref[where, lanes] + extra

    at_first = (place_ref[0] == 0).astype(jnp.int32)
    at_last = (place_ref[0] == last_place).astype(jnp.int32)
    sums = []

    def finish(num, den, halo, own):
        value = num / jnp.maximum(den, floor_value)
        row = lax.broadcasted_iota(jnp.int32, num.shape, 0)
        inside = (row >= halo * at_first) & (row < own + halo + (1 - at_last) * 4096)
        cover = jnp.where(inside, den, 0.0)
        return value, cover * value, cover

    level_one_sums = None
    for t in range(9):
        lanes = slice(t * 128, t * 128 + 128)
        value, product, cover = finish(p1_ref[:, lanes], c1_ref[:, lanes], 8, rows // 2)
        p1_ref[:, lanes] = product
        c1_ref[:, lanes] = cover
        if t < 8:
            own = slice(8, 8 + rows // 2)
            one_ref[:, lanes] = value[own]
            new = (
                jnp.sum(fold(product[own]), 0),
                jnp.sum(fold(cover[own]), 0),
                jnp.max(fold(value[own]), 0),
            )
            if level_one_sums is None:
                level_one_sums = new
            else:
                old = level_one_sums
                level_one_sums = (
                    old[0] + new[0], old[1] + new[1], jnp.maximum(old[2], new[2])
                )
    sums.append(level_one_sums)

    def next_level(p_ref, c_ref, tiles, in_rows, out_rows, halo, own_rows, out_ref, p_out, c_out):
        total = None
        nums = []
        dens = []
        for ref, dest in ((p_ref, nums), (c_ref, dens)):
            blocks = []
            for t in range(tiles):
                high, low = split(ref[:, t * 256 : t * 256 + 256])
                blocks.append(dot(high, band) + dot(low, band))
            high, low = split(ref[:, tiles * 256 : tiles * 256 + 128])
            ring = band_halo_ref[...]
            blocks.append(dot(high, ring) + dot(low, ring))
            count = tiles + 1
            for t in range(count):
                across = blocks[t][:, 0:128] + pick(
                    blocks[(t - 1) % count][:, 128:256], blocks[(t + 1) % count][:, 128:256]
                )
                slot = t % 4
                tall_ref[slot, 8 : 8 + in_rows, :] = across
                tall_ref[slot, 8 + in_rows : 2 * out_rows + 16, :] = jnp.zeros(
                    (2 * out_rows + 8 - in_rows, 128), f32
                )
                dest.append(rows_down(tall_ref, 7, out_rows, slot))
        for t in range(tiles + 1):
            value, product, cover = finish(nums[t], dens[t], halo, own_rows)
            if p_out is not None:
                p_out[:, t * 128 : t * 128 + 128] = product
                c_out[:, t * 128 : t * 128 + 128] = cover
            if t < tiles:
                own = slice(halo, halo + own_rows)
                value_ref[0, 0:out_rows, :] = value
                value_ref[1, 0:out_rows, :] = product
                value_ref[2, 0:out_rows, :] = cover
                v, p, c = (value_ref[k, own, :] for k in range(3))
                out_ref[:, t * 128 : t * 128 + 128] = v
                new = (jnp.sum(fold(p), 0), jnp.sum(fold(c), 0), jnp.max(fold(v), 0))
                total = (
                    new
                    if total is None
                    else (total[0] + new[0], total[1] + new[1], jnp.maximum(total[2], new[2]))
                )
        sums.append(total)

    next_level(p1_ref, c1_ref, 4, 272, 136, 4, 128, two_ref, p2_ref, c2_ref)
    next_level(p2_ref, c2_ref, 2, 136, 72, 2, 64, three_ref, p3_ref, c3_ref)
    next_level(p3_ref, c3_ref, 1, 72, 40, 1, 32, four_ref, None, None)

    lane = lane_iota((1, 128))
    row = jnp.zeros((1, 128), f32)
    for level in range(4):
        for kind in range(3):
            part = sums[level][kind]
            one = (jnp.max if kind == 2 else jnp.sum)(part, axis=0, keepdims=True)
            one = (jnp.max if kind == 2 else jnp.sum)(one, axis=1, keepdims=True)
            row = jnp.where(lane == kind * 4 + level, one, row)
    stats_ref[...] = jnp.broadcast_to(row, stats_ref.shape)


def all_levels(place, last_place, chips, owns, by_core, by_chip, tables, rows, cols):
    vmem = pl.BlockSpec(memory_space=pltpu.VMEM)
    shapes = [(rows >> k, cols >> k) for k in (1, 2, 3, 4)]
    outs = [pltpu.VMEM(shape, f32) for shape in shapes]
    half = rows // 2 + 16
    return pl.pallas_call(
        functools.partial(levels_kernel, last_place=last_place),
        in_specs=[pl.BlockSpec(memory_space=pltpu.SMEM)] + [vmem] * 9,
        out_specs=[vmem] * 5,
        out_shape=outs + [pltpu.VMEM((chips, 128), f32)],
        scratch_shapes=[
            pltpu.VMEM((half, cols // 2 + 128), f32),
            pltpu.VMEM((half, cols // 2 + 128), f32),
            pltpu.VMEM((136, cols // 4 + 128), f32),
            pltpu.VMEM((136, cols // 4 + 128), f32),
            pltpu.VMEM((72, cols // 8 + 128), f32),
            pltpu.VMEM((72, cols // 8 + 128), f32),
            pltpu.VMEM((4, rows + 48, 128), f32),
            pltpu.VMEM((2, 2, 9, 48, 128), f32),
            pltpu.VMEM((3, 136, 128), f32),
        ],
        compiler_params=pltpu.CompilerParams(vmem_limit_bytes=vmem_limit),
        name="all_levels",
    )(place, *owns, by_core, by_chip, *tables)


def emit_kernel(after_ref, *refs):
    del after_ref
    *refs, sems = refs
    copies = [
        pltpu.make_async_copy(refs[k], refs[k + 4], sems.at[k]) for k in range(4)
    ]
    for copy in copies:
        copy.start()
    for copy in copies:
        copy.wait()


def emit(after, levels):
    return pl.pallas_call(
        emit_kernel,
        in_specs=[pl.BlockSpec(memory_space=pltpu.VMEM)] * 5,
        out_specs=[pl.BlockSpec(memory_space=pl.ANY)] * 4,
        out_shape=[jax.ShapeDtypeStruct(level.shape, f32) for level in levels],
        scratch_shapes=[pltpu.SemaphoreType.DMA((4,))],
        compiler_params=pltpu.CompilerParams(vmem_limit_bytes=vmem_limit),
        name="emit",
    )(after, *[on_chip(level) for level in levels])


def per_device(surface_field, land_words):
    rows, cols = surface_field.shape
    row_devices = lax.axis_size(ROWS)
    col_devices = lax.axis_size(COLS)
    total_rows = rows * row_devices
    position = lax.axis_index(ROWS)

    band = jnp.asarray(band_main(), bf16)
    ring = jnp.asarray(band_halo(64, 0, 128), bf16)
    mixed = jnp.asarray(
        np.concatenate([band_halo(16, 0, 128), band_halo(16, 16, 112)], axis=1), bf16
    )

    place = jnp.reshape(position, (1,))
    words = land_words.T

    east = [(i, (i + 1) % col_devices) for i in range(col_devices)]
    west = [(target, source) for source, target in east]

    to_left, to_right, near, near_words, cosines = columns_strips(
        place, in_hbm(surface_field), in_hbm(words), total_rows
    )
    near, near_words, cosines = on_chip(near), on_chip(near_words), on_chip(cosines)
    from_right = lax.ppermute(to_left, COLS, west)
    from_left = lax.ppermute(to_right, COLS, east)
    twice = jnp.concatenate([band, band], axis=0)
    *upper, lower_near = own_level(near, near_words, cosines, twice, 0, in_hbm(surface_field))
    lower_near = on_chip(lower_near)
    to_core, to_chip, halo = rows_strips(
        place, on_chip(upper[0]), near, lower_near, near_words, on_chip(from_right), on_chip(from_left),
        cosines, (band, mixed),
    )
    by_core = lax.ppermute(to_core, ROWS, [(i, i ^ 1) for i in range(row_devices)])
    by_chip = lax.ppermute(to_chip, ROWS, [(i, ((i - 1) ^ 1) + 1) for i in range(1, row_devices - 1)])
    lower = own_level(lower_near, near_words, cosines, twice, 1, on_chip(halo), mixed)
    chips = lax.axis_size(CHIPS)
    *levels, stats = all_levels(
        place, row_devices - 1, chips, [on_chip(x) for x in (*upper, *lower)],
        on_chip(by_core), on_chip(by_chip), (band, ring), rows, cols,
    )

    is_sum = jnp.arange(128) < 8
    every = lax.all_to_all(stats, CHIPS, 0, 0, tiled=True)
    stats = jnp.where(is_sum, jnp.sum(every, axis=0), jnp.max(every, axis=0))
    other = lax.ppermute(stats, CORE, [(0, 1), (1, 0)])
    one, two, three, four = emit(on_chip(stats), levels)
    sums = stats[0:8] + other[0:8]
    maxima = jnp.maximum(stats[8:12], other[8:12])
    means = sums[0:4] / (sums[4:8] + mean_eps)
    return (one, two, three, four, means, maxima)


def solution(mesh):
    finer = Mesh(
        mesh.devices.reshape(2, 4, 2, 2, 4), ("rows_0", "rows_1", "rows_2", "cols_0", "cols_1")
    )
    in_specs = (P(ROWS, COLS), P(ROWS, COLS))
    out_specs = (P(ROWS, COLS), P(ROWS, COLS), P(ROWS, COLS), P(ROWS, COLS), P(), P())
    return jax.shard_map(
        per_device, mesh=finer, in_specs=in_specs, out_specs=out_specs, check_vma=False
    )
```

```python
import functools
import math

import jax
import jax.numpy as jnp
import numpy as np
from jax import lax
from jax.experimental import pallas as pl
from jax.experimental.pallas import tpu as pltpu
from jax.sharding import Mesh
from jax.sharding import PartitionSpec as P

ROWS = ("rows_0", "rows_1", "rows_2")
COLS = ("cols_0", "cols_1")
CHIPS = ("rows_0", "rows_1", "cols_0", "cols_1")
CORE = "rows_2"


stencil_weights = (0.125, 0.375, 0.375, 0.125)
floor_value = 0.05
mean_eps = 1e-06

vmem_limit = 20 * 1024 * 1024

f32 = jnp.float32
bf16 = jnp.bfloat16


def band_main():
    table = np.zeros((256, 256), np.float32)
    for j in range(128):
        for a in range(4):
            k = 2 * j - 1 + a
            if 0 <= k < 256:
                table[k, j] = stencil_weights[a]
    table[255, 128] = stencil_weights[0]
    table[0, 255] = stencil_weights[3]
    return table


def band_halo(width, right, left):
    table = np.zeros((128, 256), np.float32)
    for j in range(width // 2):
        for a in range(4):
            k = 2 * j - 1 + a
            if 0 <= k < width:
                table[right + k, j] = stencil_weights[a]
        for a in range(4):
            k = -3 - 2 * j + a
            if -width <= k < 0:
                table[left + k, 127 - j] = stencil_weights[a]
    table[left - 1, 128] = stencil_weights[0]
    table[right, 255] = stencil_weights[3]
    return table


def lane_iota(shape):
    return lax.broadcasted_iota(jnp.int32, shape, 1)


def words_wide(words):
    return jnp.concatenate([words, words], axis=0).T


def land_mask(wide, tile):
    lane = lane_iota(wide.shape)
    place = 4 * tile + lax.shift_right_logical(lane, 5)
    word = jnp.take_along_axis(wide, place, axis=1, mode="promise_in_bounds")
    return (word & lax.shift_left(jnp.int32(1), lane & 31)) != 0


def split(x):
    high = x.astype(bf16)
    low = (x - high.astype(f32)).astype(bf16)
    return high, low


def dot(a, b):
    return jnp.dot(a, b, preferred_element_type=f32)


def down_rows(line, count):
    return jnp.broadcast_to(line, (128, 128)).T[0:count]


def rows_down(ref, start, count, *rest):
    index = lambda a: (*rest, pl.ds(start + a, count, stride=2), slice(None))
    outer = ref[index(0)] + ref[index(3)]
    inner = ref[index(1)] + ref[index(2)]
    return stencil_weights[0] * outer + stencil_weights[1] * inner


def on_chip(x):
    return pltpu.with_memory_space_constraint(x, pltpu.VMEM)


def in_hbm(x):
    return pltpu.with_memory_space_constraint(x, pltpu.HBM)


def columns_kernel(
    place_ref, field_ref, words_ref,
    to_left_ref, to_right_ref, near_ref, near_words_ref, cos_ref,
    left_ref, right_ref, sems,
    *, total_rows,
):
    rows, cols = field_ref.shape
    small = [
        pltpu.make_async_copy(words_ref, near_words_ref, sems.at[0]),
        pltpu.make_async_copy(field_ref.at[:, 0:128], left_ref, sems.at[1]),
        pltpu.make_async_copy(field_ref.at[:, cols - 128 : cols], right_ref, sems.at[2]),
    ]
    part = rows // 4
    large = [
        pltpu.make_async_copy(
            field_ref.at[k * part : k * part + part, :],
            near_ref.at[k * part : k * part + part, :],
            sems.at[3 + k],
        )
        for k in range(2)
    ]
    for copy in small + large:
        copy.start()
    line = lax.broadcasted_iota(jnp.int32, (8, 128), 0)
    global_rows = place_ref[0] * rows + line * 128 + lane_iota((8, 128))
    latitude = ((global_rows.astype(f32) + 0.5) / total_rows - 0.5) * math.pi
    cos_ref[...] = jnp.cos(latitude)
    for copy in small:
        copy.wait()
    wide = words_wide(near_words_ref[...])
    left_mask = land_mask(wide, 0)
    right_mask = land_mask(wide, 15)
    lane = lane_iota(left_mask.shape)
    left_land = pltpu.roll(jnp.where(left_mask, 1.0, 0.0), 16, 1)
    right_land = pltpu.roll(jnp.where(right_mask, 1.0, 0.0), 112, 1)
    left_side = jnp.where(lane < 16, jnp.where(left_mask, left_ref[...], 0.0), left_land)
    right_side = jnp.where(lane >= 112, jnp.where(right_mask, right_ref[...], 0.0), right_land)
    both = jnp.where(lane < 64, left_side, right_side).T
    to_left_ref[...] = both[0:32]
    to_right_ref[...] = both[96:128]
    for copy in large:
        copy.wait()


def columns_strips(place, field, words, total_rows):
    rows, cols = field.shape
    return pl.pallas_call(
        functools.partial(columns_kernel, total_rows=total_rows),
        in_specs=[pl.BlockSpec(memory_space=pltpu.SMEM)] + [pl.BlockSpec(memory_space=pl.ANY)] * 2,
        out_specs=[pl.BlockSpec(memory_space=pltpu.VMEM)] * 5,
        out_shape=[
            pltpu.VMEM((32, rows), f32),
            pltpu.VMEM((32, rows), f32),
            pltpu.VMEM((rows // 2, cols), f32),
            pltpu.VMEM(words.shape, words.dtype),
            pltpu.VMEM((8, 128), f32),
        ],
        scratch_shapes=[
            pltpu.VMEM((rows, 128), f32),
            pltpu.VMEM((rows, 128), f32),
            pltpu.SemaphoreType.DMA((5,)),
        ],
        compiler_params=pltpu.CompilerParams(vmem_limit_bytes=vmem_limit),
        name="columns_strips",
    )(place, field, words)


def rows_kernel(
    place_ref, after_ref, upper_ref, lower_ref, words_ref, right_ref, left_ref,
    cos_ref, band_ref, mixed_ref,
    to_core_ref, to_chip_ref, halo_ref, wide_ref, lhs_ref, corner_ref,
):
    del after_ref
    rows = halo_ref.shape[0]
    height = lower_ref.shape[0]
    for part in range(rows // 128):
        cols = slice(part * 128, part * 128 + 128)
        halo_ref[cols, :] = jnp.concatenate(
            [right_ref[:, cols], jnp.zeros((64, 128), f32), left_ref[:, cols]], axis=0
        ).T
    odd = place_ref[0] & 1
    cos_top = down_rows(cos_ref[0:1, :], 16)
    cos_bottom = down_rows(cos_ref[3:4, :], 128)[112:128]
    sides = ((to_core_ref, 1 - odd), (to_chip_ref, odd))
    for side, (_, bottom) in enumerate(sides):
        first = pl.multiple_of(bottom * (rows - 16), 16)
        wide_ref[...] = words_wide(words_ref[:, pl.ds(pl.multiple_of(bottom * (rows - 128), 128), 128)])
        wide = wide_ref[pl.ds(pl.multiple_of(bottom * 112, 16), 16), :]
        for tile in range(16):
            lanes = slice(tile * 128, tile * 128 + 128)
            half = slice(tile % 2 * 128, tile % 2 * 128 + 128)
            mask = land_mask(wide, tile)
            field = jnp.where(
                bottom == 1, lower_ref[height - 16 : height, lanes], upper_ref[0:16, lanes]
            )
            high, low = split(jnp.where(mask, field, 0.0))
            land = jnp.where(mask, 1.0, 0.0).astype(bf16)
            base = side * 384 + tile // 2 * 48
            for k, value in enumerate((high, low, land)):
                lhs_ref[base + k * 16 : base + k * 16 + 16, half] = value
        high, low = split(halo_ref[pl.ds(first, 16), :])
        corner_ref[side * 32 : side * 32 + 16, :] = high
        corner_ref[side * 32 + 16 : side * 32 + 32, :] = low
    across = dot(lhs_ref[...], band_ref[...])
    corners = dot(corner_ref[...], mixed_ref[...])
    low_half = lane_iota((16, 128)) < 64
    for side, (out_ref, bottom) in enumerate(sides):
        cos = jnp.where(bottom == 1, cos_bottom, cos_top)
        corner = corners[side * 32 : side * 32 + 16] + corners[side * 32 + 16 : side * 32 + 32]
        for which in range(2):
            parts = []
            for t in range(8):
                base = side * 384 + t * 48
                if which == 0:
                    parts.append(across[base : base + 16] + across[base + 16 : base + 32])
                else:
                    parts.append(across[base + 32 : base + 48])
            parts.append(corner[:, which * 256 : which * 256 + 256])
            for t in range(9):
                edges = jnp.where(
                    low_half, parts[(t - 1) % 9][:, 128:256], parts[(t + 1) % 9][:, 128:256]
                )
                out_ref[which * 16 : which * 16 + 16, t * 128 : t * 128 + 128] = (
                    parts[t][:, 0:128] + edges
                ) * cos


def rows_strips(place, after, upper, lower, words, from_right, from_left, cosines, tables):
    rows, cols = words.shape[1], upper.shape[1]
    return pl.pallas_call(
        rows_kernel,
        in_specs=[pl.BlockSpec(memory_space=pltpu.SMEM)]
        + [pl.BlockSpec(memory_space=pltpu.VMEM)] * 9,
        out_specs=[pl.BlockSpec(memory_space=pltpu.VMEM)] * 3,
        out_shape=[
            pltpu.VMEM((32, cols // 2 + 128), f32),
            pltpu.VMEM((32, cols // 2 + 128), f32),
            pltpu.VMEM((rows, 128), f32),
        ],
        scratch_shapes=[
            pltpu.VMEM((128, 128), jnp.int32),
            pltpu.VMEM((768, 256), bf16),
            pltpu.VMEM((64, 128), bf16),
        ],
        compiler_params=pltpu.CompilerParams(vmem_limit_bytes=vmem_limit),
        name="rows_strips",
    )(place, after, upper, lower, words, from_right, from_left, cosines, *tables)


def fold(x):
    return x.reshape(x.shape[0] // 8, 8, 128)


def side_terms(halo_ref, cos_ref, mixed_ref, side_ref, tall_ref):
    rows = halo_ref.shape[0]
    tall_ref[:, 0:24, :] = jnp.zeros((4, 24, 128), f32)
    tall_ref[:, 24 + rows :, :] = jnp.zeros((4, 24, 128), f32)
    mixed = mixed_ref[...]
    for part in range(rows // 128):
        high, low = split(halo_ref[part * 128 : part * 128 + 128, :])
        across = dot(high, mixed) + dot(low, mixed)
        cos = down_rows(cos_ref[part : part + 1, :], 128)
        for k in range(4):
            tall_ref[k, 24 + part * 128 : 152 + part * 128, :] = (
                across[:, k * 128 : k * 128 + 128] * cos
            )
    for k in range(4):
        side_ref[k] = rows_down(tall_ref, 7, side_ref.shape[1], k)


def lower_kernel(
    halo_ref, mixed_ref, num_a_ref, den_a_ref, field_ref, words_ref, cos_ref, band_ref,
    p1_ref, c1_ref, one_ref, part_ref, *scratch, skip,
):
    *scratch, num_b_ref, den_b_ref, side_ref, tall_ref = scratch

    @pl.when(pl.program_id(0) == 0)
    def _():
        side_terms(halo_ref, cos_ref, mixed_ref, side_ref, tall_ref)

    upper_kernel(field_ref, words_ref, cos_ref, band_ref, num_b_ref, den_b_ref, *scratch, skip=skip)

    @pl.when(pl.program_id(0) == pl.num_programs(0) - 1)
    def _():
        count = p1_ref.shape[0]
        mid = num_a_ref.shape[0] - 16
        part = [jnp.zeros((8, 128), f32), jnp.zeros((8, 128), f32), jnp.full((8, 128), -jnp.inf, f32)]
        for t in range(9):
            lanes = slice(t * 128, t * 128 + 128)
            sums = []
            for k, (a_ref, b_ref) in enumerate(((num_a_ref, num_b_ref), (den_a_ref, den_b_ref))):
                whole = jnp.concatenate(
                    [
                        a_ref[0:mid, lanes],
                        a_ref[mid : mid + 16, lanes] + b_ref[0:16, lanes],
                        b_ref[16 : mid + 16, lanes],
                    ],
                    axis=0,
                )
                if t == 8:
                    whole = whole + side_ref[2 * k]
                elif t in (0, 7):
                    edge = side_ref[2 * k + 1]
                    before = lane_iota(edge.shape) < 64
                    whole = whole + jnp.where(before == (t == 0), edge, 0.0)
                sums.append(whole)
            num, den = sums
            value = num / jnp.maximum(den, floor_value)
            product = den * value
            inner = slice(16, count - 16)
            p1_ref[0:16, lanes] = num[0:16]
            p1_ref[inner, lanes] = product[inner]
            p1_ref[count - 16 : count, lanes] = num[count - 16 : count]
            c1_ref[:, lanes] = den
            if t < 8:
                one_ref[8 : count - 24, lanes] = value[inner]
                part[0] = part[0] + jnp.sum(fold(product[inner]), 0)
                part[1] = part[1] + jnp.sum(fold(den[inner]), 0)
                part[2] = jnp.maximum(part[2], jnp.max(fold(value[inner]), 0))
        for k in range(3):
            part_ref[k] = part[k]


def first_kernel(
    whole_ref, field_ref, words_ref, cos_ref, band_ref,
    num_ref, den_ref, lower_ref, *scratch, skip,
):
    height = lower_ref.shape[0]
    copy = pltpu.make_async_copy(
        whole_ref.at[height : 2 * height, :], lower_ref, scratch[-1].at[0]
    )

    @pl.when(pl.program_id(0) == 0)
    def _():
        copy.start()

    upper_kernel(field_ref, words_ref, cos_ref, band_ref, num_ref, den_ref, *scratch[:-1], skip=skip)

    @pl.when(pl.program_id(0) == pl.num_programs(0) - 1)
    def _():
        copy.wait()


def upper_kernel(
    field_ref, words_ref, cos_ref, band_ref, num_ref, den_ref,
    product_ref, cover_ref, main_ref, edge_ref, sheet_ref,
    *, skip,
):
    step = pl.program_id(0)
    blocks = pl.num_programs(0) - 1
    height = field_ref.shape[0] // blocks
    origin = pl.multiple_of(step * height, 128)
    line = pl.multiple_of((skip + step) * height, 128)

    @pl.when(step == 0)
    def _():
        sheet_ref[:, :, 0:24, :] = jnp.zeros((2, 9, 24, 128), f32)
        sheet_ref[:, :, 24 + 2 * height :, :] = jnp.zeros(
            (2, 9, sheet_ref.shape[2] - 24 - 2 * height, 128), f32
        )

    @pl.when(step < blocks)
    def _():
        wide = words_wide(words_ref[:, pl.ds(line, height)])
        for tile in range(8):
            part = slice(tile * height, tile * height + height)
            for half in range(2):
                lanes = slice(tile * 256 + half * 128, tile * 256 + half * 128 + 128)
                mask = land_mask(wide, 2 * tile + half)
                high, low = split(
                    jnp.where(mask, field_ref[pl.ds(origin, height), lanes], 0.0)
                )
                product_ref[part, half * 128 : half * 128 + 128] = high
                product_ref[part, 256 + half * 128 : 384 + half * 128] = low
                cover_ref[part, half * 128 : half * 128 + 128] = jnp.where(mask, 1.0, 0.0).astype(
                    bf16
                )
        cos = down_rows(cos_ref[pl.ds(skip + step, 1), :], 128)
        low_half = lane_iota((height, 128)) < 64
        start = pl.multiple_of(24 + step * height, 8)
        for which, (lhs_ref, depth) in enumerate(((product_ref, 512), (cover_ref, 256))):
            across = dot(lhs_ref[...], band_ref[0:depth, :])
            main_ref[...] = across[:, 0:128]
            edge_ref[...] = across[:, 128:256]
            zero = jnp.zeros((height, 128), f32)
            for t in range(9):
                get = lambda ref, k: ref[k * height : k * height + height, :]
                main = get(main_ref, t) if t < 8 else zero
                before = get(edge_ref, t - 1) if t > 0 else zero
                after = get(edge_ref, (t + 1) % 9) if t != 7 else zero
                sheet_ref[which, t, pl.ds(start, height), :] = (
                    main + jnp.where(low_half, before, after)
                ) * cos

    def down(count):
        first = 7 + step * height
        place = pl.multiple_of(step * (height // 2), 8)
        for which, out_ref in ((0, num_ref), (1, den_ref)):
            for t in range(9):
                out_ref[pl.ds(place, count), t * 128 : t * 128 + 128] = rows_down(
                    sheet_ref, first, count, which, t
                )

    @pl.when(step < blocks)
    def _():
        down(height // 2)

    @pl.when(step == blocks)
    def _():
        down(16)


def own_level(field, words, cosines, band, part, *beside):
    height = 128
    blocks = field.shape[0] // height
    rows, cols = 2 * field.shape[0], field.shape[1]
    skip = part * blocks
    vmem = pl.BlockSpec(memory_space=pltpu.VMEM)
    half = pltpu.VMEM((blocks * height // 2 + 16, cols // 2 + 128), f32)
    if part == 0:
        kernel, given = first_kernel, [pl.BlockSpec(memory_space=pl.ANY)]
        outs = [half, half, pltpu.VMEM(field.shape, f32)]
        scratch = [pltpu.SemaphoreType.DMA((1,))]
    else:
        kernel, given = lower_kernel, [vmem] * 4
        level = pltpu.VMEM((rows // 2 + 16, cols // 2 + 128), f32)
        outs = [level, level, pltpu.VMEM((rows // 2, cols // 2), f32), pltpu.VMEM((3, 8, 128), f32)]
        scratch = [
            half,
            half,
            pltpu.VMEM((4, rows // 2 + 16, 128), f32),
            pltpu.VMEM((4, rows + 48, 128), f32),
        ]
    return pl.pallas_call(
        functools.partial(kernel, skip=skip),
        grid=(blocks + 1,),
        in_specs=given + [vmem] * 4,
        out_specs=[vmem] * len(outs),
        out_shape=outs,
        scratch_shapes=[
            pltpu.VMEM((8 * height, 512), bf16),
            pltpu.VMEM((8 * height, 256), bf16),
            pltpu.VMEM((8 * height, 128), f32),
            pltpu.VMEM((8 * height, 128), f32),
            pltpu.VMEM((2, 9, 24 + (blocks + 1) * height, 128), f32),
            *scratch,
        ],
        compiler_params=pltpu.CompilerParams(vmem_limit_bytes=vmem_limit),
        name="own_level",
    )(*beside, field, words, cosines, band)


def levels_kernel(
    place_ref, p1_ref, c1_ref, part_ref, core_ref, chip_ref, band_ref, band_halo_ref,
    head_ref, tail_ref, two_ref, three_ref, four_ref, stats_ref,
    ends_ref, p2_ref, c2_ref, p3_ref, c3_ref, tall_ref, strip_ref, value_ref,
    *, last_place,
):
    count = p1_ref.shape[0]
    rows = 2 * (count - 16)
    band = band_ref[...]
    odd = (place_ref[0] & 1) == 1
    tall_ref[:, 0:8, :] = jnp.zeros((4, 8, 128), f32)

    def pick(before, after):
        shape = before.shape
        return jnp.where(lane_iota(shape) < 64, before, after)

    strip_ref[...] = jnp.zeros(strip_ref.shape, f32)
    for side, first in ((0, 8), (1, 24)):
        of_core = odd if side == 0 else jnp.logical_not(odd)
        strip = jnp.where(of_core, core_ref[...], chip_ref[...])
        for which in range(2):
            for t in range(9):
                strip_ref[side, which, t, first : first + 16, :] = strip[
                    which * 16 : which * 16 + 16, t * 128 : t * 128 + 128
                ]

    at_first = (place_ref[0] == 0).astype(jnp.int32)
    at_last = (place_ref[0] == last_place).astype(jnp.int32)
    sums = []

    def finish(num, den, halo, own):
        value = num / jnp.maximum(den, floor_value)
        row = lax.broadcasted_iota(jnp.int32, num.shape, 0)
        inside = (row >= halo * at_first) & (row < own + halo + (1 - at_last) * 4096)
        cover = jnp.where(inside, den, 0.0)
        return value, cover * value, cover

    level_one_sums = tuple(part_ref[k] for k in range(3))
    row = lax.broadcasted_iota(jnp.int32, (16, 128), 0)
    for side in range(2):
        where = slice(0, 16) if side == 0 else slice(count - 16, count)
        own = slice(8, 16) if side == 0 else slice(0, 8)
        inside = (row >= 8 * at_first) if side == 0 else (row < 8 + (1 - at_last) * 8)
        out_ref = head_ref if side == 0 else tail_ref
        for t in range(9):
            lanes = slice(t * 128, t * 128 + 128)
            num = p1_ref[where, lanes] + rows_down(strip_ref, 7, 16, side, 0, t)
            den = c1_ref[where, lanes] + rows_down(strip_ref, 7, 16, side, 1, t)
            value = num / jnp.maximum(den, floor_value)
            cover = jnp.where(inside, den, 0.0)
            product = cover * value
            ends_ref[side, 0, :, lanes] = product
            ends_ref[side, 1, :, lanes] = cover
            if t < 8:
                out_ref[:, lanes] = value[own]
                old = level_one_sums
                level_one_sums = (
                    old[0] + product[own], old[1] + cover[own], jnp.maximum(old[2], value[own])
                )
    sums.append(level_one_sums)

    def next_level(p_ref, c_ref, tiles, in_rows, out_rows, halo, own_rows, out_ref, p_out, c_out):
        total = None
        nums = []
        dens = []
        for which, (ref, dest) in enumerate(((p_ref, nums), (c_ref, dens))):
            blocks = []

            def part(first, width):
                lanes = slice(first, first + width)
                if ref.shape[0] != count:
                    return ref[:, lanes]
                ends = [ends_ref[side, which, :, lanes] for side in range(2)]
                return jnp.concatenate([ends[0], ref[16 : count - 16, lanes], ends[1]], axis=0)

            for t in range(tiles):
                high, low = split(part(t * 256, 256))
                blocks.append(dot(high, band) + dot(low, band))
            high, low = split(part(tiles * 256, 128))
            ring = band_halo_ref[...]
            blocks.append(dot(high, ring) + dot(low, ring))
            ring_tiles = tiles + 1
            for t in range(ring_tiles):
                across = blocks[t][:, 0:128] + pick(
                    blocks[(t - 1) % ring_tiles][:, 128:256],
                    blocks[(t + 1) % ring_tiles][:, 128:256],
                )
                slot = t % 4
                tall_ref[slot, 8 : 8 + in_rows, :] = across
                tall_ref[slot, 8 + in_rows : 2 * out_rows + 16, :] = jnp.zeros(
                    (2 * out_rows + 8 - in_rows, 128), f32
                )
                dest.append(rows_down(tall_ref, 7, out_rows, slot))
        for t in range(tiles + 1):
            value, product, cover = finish(nums[t], dens[t], halo, own_rows)
            if p_out is not None:
                p_out[:, t * 128 : t * 128 + 128] = product
                c_out[:, t * 128 : t * 128 + 128] = cover
            if t < tiles:
                own = slice(halo, halo + own_rows)
                value_ref[0, 0:out_rows, :] = value
                value_ref[1, 0:out_rows, :] = product
                value_ref[2, 0:out_rows, :] = cover
                v, p, c = (value_ref[k, own, :] for k in range(3))
                out_ref[:, t * 128 : t * 128 + 128] = v
                new = (jnp.sum(fold(p), 0), jnp.sum(fold(c), 0), jnp.max(fold(v), 0))
                total = (
                    new
                    if total is None
                    else (total[0] + new[0], total[1] + new[1], jnp.maximum(total[2], new[2]))
                )
        sums.append(total)

    next_level(p1_ref, c1_ref, 4, 272, 136, 4, 128, two_ref, p2_ref, c2_ref)
    next_level(p2_ref, c2_ref, 2, 136, 72, 2, 64, three_ref, p3_ref, c3_ref)
    next_level(p3_ref, c3_ref, 1, 72, 40, 1, 32, four_ref, None, None)

    lane = lane_iota((1, 128))
    row = jnp.zeros((1, 128), f32)
    for level in range(4):
        for kind in range(3):
            part = sums[level][kind]
            one = (jnp.max if kind == 2 else jnp.sum)(part, axis=0, keepdims=True)
            one = (jnp.max if kind == 2 else jnp.sum)(one, axis=1, keepdims=True)
            row = jnp.where(lane == kind * 4 + level, one, row)
    stats_ref[...] = jnp.broadcast_to(row, stats_ref.shape)


def all_levels(place, last_place, chips, level_one, by_core, by_chip, tables, rows, cols):
    vmem = pl.BlockSpec(memory_space=pltpu.VMEM)
    shapes = [(8, cols // 2)] * 2 + [(rows >> k, cols >> k) for k in (2, 3, 4)]
    outs = [pltpu.VMEM(shape, f32) for shape in shapes]
    return pl.pallas_call(
        functools.partial(levels_kernel, last_place=last_place),
        in_specs=[pl.BlockSpec(memory_space=pltpu.SMEM)] + [vmem] * 7,
        out_specs=[vmem] * 6,
        out_shape=outs + [pltpu.VMEM((chips, 128), f32)],
        scratch_shapes=[
            pltpu.VMEM((2, 2, 16, cols // 2 + 128), f32),
            pltpu.VMEM((136, cols // 4 + 128), f32),
            pltpu.VMEM((136, cols // 4 + 128), f32),
            pltpu.VMEM((72, cols // 8 + 128), f32),
            pltpu.VMEM((72, cols // 8 + 128), f32),
            pltpu.VMEM((4, rows + 48, 128), f32),
            pltpu.VMEM((2, 2, 9, 48, 128), f32),
            pltpu.VMEM((3, 136, 128), f32),
        ],
        compiler_params=pltpu.CompilerParams(vmem_limit_bytes=vmem_limit),
        name="all_levels",
    )(place, *level_one, by_core, by_chip, *tables)


def emit_kernel(
    after_ref, one_ref, head_ref, tail_ref, two_ref, three_ref, four_ref,
    one_out, two_out, three_out, four_out, sems,
):
    del after_ref
    count = one_ref.shape[0]
    pairs = (
        (one_ref.at[8 : count - 8, :], one_out.at[8 : count - 8, :]),
        (head_ref, one_out.at[0:8, :]),
        (tail_ref, one_out.at[count - 8 : count, :]),
        (two_ref, two_out),
        (three_ref, three_out),
        (four_ref, four_out),
    )
    copies = [pltpu.make_async_copy(*pair, sems.at[k]) for k, pair in enumerate(pairs)]
    for copy in copies:
        copy.start()
    for copy in copies:
        copy.wait()


def emit(after, one, head, tail, *rest):
    levels = (one, *rest)
    return pl.pallas_call(
        emit_kernel,
        in_specs=[pl.BlockSpec(memory_space=pltpu.VMEM)] * 7,
        out_specs=[pl.BlockSpec(memory_space=pl.ANY)] * 4,
        out_shape=[jax.ShapeDtypeStruct(level.shape, f32) for level in levels],
        scratch_shapes=[pltpu.SemaphoreType.DMA((6,))],
        compiler_params=pltpu.CompilerParams(vmem_limit_bytes=vmem_limit),
        name="emit",
    )(after, *[on_chip(level) for level in (one, head, tail, *rest)])


def per_device(surface_field, land_words):
    rows, cols = surface_field.shape
    row_devices = lax.axis_size(ROWS)
    col_devices = lax.axis_size(COLS)
    total_rows = rows * row_devices
    position = lax.axis_index(ROWS)

    band = jnp.asarray(band_main(), bf16)
    ring = jnp.asarray(band_halo(64, 0, 128), bf16)
    mixed = jnp.asarray(
        np.concatenate([band_halo(16, 0, 128), band_halo(16, 16, 112)], axis=1), bf16
    )

    place = jnp.reshape(position, (1,))
    words = land_words.T

    east = [(i, (i + 1) % col_devices) for i in range(col_devices)]
    west = [(target, source) for source, target in east]

    to_left, to_right, near, near_words, cosines = columns_strips(
        place, in_hbm(surface_field), in_hbm(words), total_rows
    )
    near, near_words, cosines = on_chip(near), on_chip(near_words), on_chip(cosines)
    from_right = lax.ppermute(to_left, COLS, west)
    from_left = lax.ppermute(to_right, COLS, east)
    twice = jnp.concatenate([band, band], axis=0)
    *upper, lower_near = own_level(near, near_words, cosines, twice, 0, in_hbm(surface_field))
    lower_near = on_chip(lower_near)
    to_core, to_chip, halo = rows_strips(
        place, on_chip(upper[0]), near, lower_near, near_words, on_chip(from_right), on_chip(from_left),
        cosines, (band, mixed),
    )
    by_chip = lax.ppermute(to_chip, ROWS, [(i, ((i - 1) ^ 1) + 1) for i in range(1, row_devices - 1)])
    by_core = lax.ppermute(to_core, ROWS, [(i, i ^ 1) for i in range(row_devices)])
    p1, c1, one, part = own_level(
        lower_near, near_words, cosines, twice, 1,
        on_chip(halo), mixed, *[on_chip(x) for x in upper],
    )
    chips = lax.axis_size(CHIPS)
    *levels, stats = all_levels(
        place, row_devices - 1, chips, [on_chip(x) for x in (p1, c1, part)],
        on_chip(by_core), on_chip(by_chip), (band, ring), rows, cols,
    )

    is_sum = jnp.arange(128) < 8
    every = lax.all_to_all(stats, CHIPS, 0, 0, tiled=True)
    stats = jnp.where(is_sum, jnp.sum(every, axis=0), jnp.max(every, axis=0))
    other = lax.ppermute(stats, CORE, [(0, 1), (1, 0)])
    one, two, three, four = emit(on_chip(stats), one, *levels)
    sums = stats[0:8] + other[0:8]
    maxima = jnp.maximum(stats[8:12], other[8:12])
    means = sums[0:4] / (sums[4:8] + mean_eps)
    return (one, two, three, four, means, maxima)


def solution(mesh):
    finer = Mesh(
        mesh.devices.reshape(2, 4, 2, 2, 4), ("rows_0", "rows_1", "rows_2", "cols_0", "cols_1")
    )
    in_specs = (P(ROWS, COLS), P(ROWS, COLS))
    out_specs = (P(ROWS, COLS), P(ROWS, COLS), P(ROWS, COLS), P(ROWS, COLS), P(), P())
    return jax.shard_map(
        per_device, mesh=finer, in_specs=in_specs, out_specs=out_specs, check_vma=False
    )
```

```python
import functools
import math

import jax
import jax.numpy as jnp
import numpy as np
from jax import lax
from jax.experimental import pallas as pl
from jax.experimental.pallas import tpu as pltpu
from jax.sharding import Mesh
from jax.sharding import PartitionSpec as P

ROWS = ("rows_0", "rows_1", "rows_2")
COLS = ("cols_0", "cols_1")
CHIPS = ("rows_0", "rows_1", "cols_0", "cols_1")
CORE = "rows_2"


stencil_weights = (0.125, 0.375, 0.375, 0.125)
floor_value = 0.05
mean_eps = 1e-06

vmem_limit = 20 * 1024 * 1024

f32 = jnp.float32
bf16 = jnp.bfloat16


def band_main():
    table = np.zeros((256, 256), np.float32)
    for j in range(128):
        for a in range(4):
            k = 2 * j - 1 + a
            if 0 <= k < 256:
                table[k, j] = stencil_weights[a]
    table[255, 128] = stencil_weights[0]
    table[0, 255] = stencil_weights[3]
    return table


def band_halo(width, right, left):
    table = np.zeros((128, 256), np.float32)
    for j in range(width // 2):
        for a in range(4):
            k = 2 * j - 1 + a
            if 0 <= k < width:
                table[right + k, j] = stencil_weights[a]
        for a in range(4):
            k = -3 - 2 * j + a
            if -width <= k < 0:
                table[left + k, 127 - j] = stencil_weights[a]
    table[left - 1, 128] = stencil_weights[0]
    table[right, 255] = stencil_weights[3]
    return table


def lane_iota(shape):
    return lax.broadcasted_iota(jnp.int32, shape, 1)


def words_wide(words):
    return jnp.concatenate([words, words], axis=0).T


def land_mask(wide, tile):
    lane = lane_iota(wide.shape)
    place = 4 * tile + lax.shift_right_logical(lane, 5)
    word = jnp.take_along_axis(wide, place, axis=1, mode="promise_in_bounds")
    return (word & lax.shift_left(jnp.int32(1), lane & 31)) != 0


def split(x):
    high = x.astype(bf16)
    low = (x - high.astype(f32)).astype(bf16)
    return high, low


def split_pair(x):
    return jnp.concatenate(split(x), axis=1)


def dot(a, b):
    return jnp.dot(a, b, preferred_element_type=f32)


def down_rows(line, count):
    return jnp.broadcast_to(line, (128, 128)).T[0:count]


def rows_down(ref, start, count, *rest):
    index = lambda a: (*rest, pl.ds(start + a, count, stride=2), slice(None))
    outer = ref[index(0)] + ref[index(3)]
    inner = ref[index(1)] + ref[index(2)]
    return stencil_weights[0] * outer + stencil_weights[1] * inner


def on_chip(x):
    return pltpu.with_memory_space_constraint(x, pltpu.VMEM)


def in_hbm(x):
    return pltpu.with_memory_space_constraint(x, pltpu.HBM)


def columns_kernel(
    place_ref, field_ref, words_ref,
    to_left_ref, to_right_ref, near_ref, near_words_ref, cos_ref,
    left_ref, right_ref, sems,
    *, total_rows,
):
    rows, cols = field_ref.shape
    small = [
        pltpu.make_async_copy(words_ref, near_words_ref, sems.at[0]),
        pltpu.make_async_copy(field_ref.at[:, 0:128], left_ref, sems.at[1]),
        pltpu.make_async_copy(field_ref.at[:, cols - 128 : cols], right_ref, sems.at[2]),
    ]
    part = rows // 4
    large = [
        pltpu.make_async_copy(
            field_ref.at[k * part : k * part + part, :],
            near_ref.at[k * part : k * part + part, :],
            sems.at[3 + k],
        )
        for k in range(2)
    ]
    for copy in small + large:
        copy.start()
    line = lax.broadcasted_iota(jnp.int32, (8, 128), 0)
    global_rows = place_ref[0] * rows + line * 128 + lane_iota((8, 128))
    latitude = ((global_rows.astype(f32) + 0.5) / total_rows - 0.5) * math.pi
    cos_ref[...] = jnp.cos(latitude)
    for copy in small:
        copy.wait()
    wide = words_wide(near_words_ref[...])
    left_mask = land_mask(wide, 0)
    right_mask = land_mask(wide, 15)
    lane = lane_iota(left_mask.shape)
    left_land = pltpu.roll(jnp.where(left_mask, 1.0, 0.0), 16, 1)
    right_land = pltpu.roll(jnp.where(right_mask, 1.0, 0.0), 112, 1)
    left_side = jnp.where(lane < 16, jnp.where(left_mask, left_ref[...], 0.0), left_land)
    right_side = jnp.where(lane >= 112, jnp.where(right_mask, right_ref[...], 0.0), right_land)
    both = jnp.where(lane < 64, left_side, right_side).T
    to_left_ref[...] = both[0:32]
    to_right_ref[...] = both[96:128]
    for copy in large:
        copy.wait()


def columns_strips(place, field, words, total_rows):
    rows, cols = field.shape
    return pl.pallas_call(
        functools.partial(columns_kernel, total_rows=total_rows),
        in_specs=[pl.BlockSpec(memory_space=pltpu.SMEM)] + [pl.BlockSpec(memory_space=pl.ANY)] * 2,
        out_specs=[pl.BlockSpec(memory_space=pltpu.VMEM)] * 5,
        out_shape=[
            pltpu.VMEM((32, rows), f32),
            pltpu.VMEM((32, rows), f32),
            pltpu.VMEM((rows // 2, cols), f32),
            pltpu.VMEM(words.shape, words.dtype),
            pltpu.VMEM((8, 128), f32),
        ],
        scratch_shapes=[
            pltpu.VMEM((rows, 128), f32),
            pltpu.VMEM((rows, 128), f32),
            pltpu.SemaphoreType.DMA((5,)),
        ],
        compiler_params=pltpu.CompilerParams(vmem_limit_bytes=vmem_limit),
        name="columns_strips",
    )(place, field, words)


def rows_kernel(
    place_ref, after_ref, upper_ref, lower_ref, words_ref, right_ref, left_ref,
    cos_ref, band_ref, mixed_ref,
    to_core_ref, to_chip_ref, halo_ref, wide_ref, lhs_ref, corner_ref,
):
    del after_ref
    rows = halo_ref.shape[0]
    height = lower_ref.shape[0]
    for part in range(rows // 128):
        cols = slice(part * 128, part * 128 + 128)
        halo_ref[cols, :] = jnp.concatenate(
            [right_ref[:, cols], jnp.zeros((64, 128), f32), left_ref[:, cols]], axis=0
        ).T
    odd = place_ref[0] & 1
    cos_top = down_rows(cos_ref[0:1, :], 16)
    cos_bottom = down_rows(cos_ref[3:4, :], 128)[112:128]
    sides = ((to_core_ref, 1 - odd), (to_chip_ref, odd))
    for side, (_, bottom) in enumerate(sides):
        first = pl.multiple_of(bottom * (rows - 16), 16)
        wide_ref[...] = words_wide(words_ref[:, pl.ds(pl.multiple_of(bottom * (rows - 128), 128), 128)])
        wide = wide_ref[pl.ds(pl.multiple_of(bottom * 112, 16), 16), :]
        for tile in range(16):
            lanes = slice(tile * 128, tile * 128 + 128)
            half = slice(tile % 2 * 128, tile % 2 * 128 + 128)
            mask = land_mask(wide, tile)
            field = jnp.where(
                bottom == 1, lower_ref[height - 16 : height, lanes], upper_ref[0:16, lanes]
            )
            high, low = split(jnp.where(mask, field, 0.0))
            land = jnp.where(mask, 1.0, 0.0).astype(bf16)
            base = side * 384 + tile // 2 * 48
            for k, value in enumerate((high, low, land)):
                lhs_ref[base + k * 16 : base + k * 16 + 16, half] = value
        high, low = split(halo_ref[pl.ds(first, 16), :])
        corner_ref[side * 32 : side * 32 + 16, :] = high
        corner_ref[side * 32 + 16 : side * 32 + 32, :] = low
    across = dot(lhs_ref[...], band_ref[...])
    corners = dot(corner_ref[...], mixed_ref[...])
    low_half = lane_iota((16, 128)) < 64
    for side, (out_ref, bottom) in enumerate(sides):
        cos = jnp.where(bottom == 1, cos_bottom, cos_top)
        corner = corners[side * 32 : side * 32 + 16] + corners[side * 32 + 16 : side * 32 + 32]
        for which in range(2):
            parts = []
            for t in range(8):
                base = side * 384 + t * 48
                if which == 0:
                    parts.append(across[base : base + 16] + across[base + 16 : base + 32])
                else:
                    parts.append(across[base + 32 : base + 48])
            parts.append(corner[:, which * 256 : which * 256 + 256])
            for t in range(9):
                edges = jnp.where(
                    low_half, parts[(t - 1) % 9][:, 128:256], parts[(t + 1) % 9][:, 128:256]
                )
                out_ref[which * 16 : which * 16 + 16, t * 128 : t * 128 + 128] = (
                    parts[t][:, 0:128] + edges
                ) * cos


def rows_strips(place, after, upper, lower, words, from_right, from_left, cosines, tables):
    rows, cols = words.shape[1], upper.shape[1]
    return pl.pallas_call(
        rows_kernel,
        in_specs=[pl.BlockSpec(memory_space=pltpu.SMEM)]
        + [pl.BlockSpec(memory_space=pltpu.VMEM)] * 9,
        out_specs=[pl.BlockSpec(memory_space=pltpu.VMEM)] * 3,
        out_shape=[
            pltpu.VMEM((32, cols // 2 + 128), f32),
            pltpu.VMEM((32, cols // 2 + 128), f32),
            pltpu.VMEM((rows, 128), f32),
        ],
        scratch_shapes=[
            pltpu.VMEM((128, 128), jnp.int32),
            pltpu.VMEM((768, 256), bf16),
            pltpu.VMEM((64, 128), bf16),
        ],
        compiler_params=pltpu.CompilerParams(vmem_limit_bytes=vmem_limit),
        name="rows_strips",
    )(place, after, upper, lower, words, from_right, from_left, cosines, *tables)


def fold(x):
    return x.reshape(x.shape[0] // 8, 8, 128)


def side_terms(halo_ref, cos_ref, mixed_ref, side_ref, tall_ref):
    rows = halo_ref.shape[0]
    tall_ref[:, 0:24, :] = jnp.zeros((4, 24, 128), f32)
    tall_ref[:, 24 + rows :, :] = jnp.zeros((4, 24, 128), f32)
    mixed = mixed_ref[...]
    for part in range(rows // 128):
        across = dot(split_pair(halo_ref[part * 128 : part * 128 + 128, :]), mixed)
        cos = down_rows(cos_ref[part : part + 1, :], 128)
        for k in range(4):
            tall_ref[k, 24 + part * 128 : 152 + part * 128, :] = (
                across[:, k * 128 : k * 128 + 128] * cos
            )
    for k in range(4):
        side_ref[k] = rows_down(tall_ref, 7, side_ref.shape[1], k)


def lower_kernel(
    halo_ref, mixed_ref, num_a_ref, den_a_ref, field_ref, words_ref, cos_ref, band_ref,
    p1_ref, c1_ref, one_ref, part_ref, *scratch, skip,
):
    *scratch, num_b_ref, den_b_ref, side_ref, tall_ref = scratch

    @pl.when(pl.program_id(0) == 0)
    def _():
        side_terms(halo_ref, cos_ref, mixed_ref, side_ref, tall_ref)

    upper_kernel(field_ref, words_ref, cos_ref, band_ref, num_b_ref, den_b_ref, *scratch, skip=skip)

    @pl.when(pl.program_id(0) == pl.num_programs(0) - 1)
    def _():
        count = p1_ref.shape[0]
        mid = num_a_ref.shape[0] - 16
        part = [jnp.zeros((8, 128), f32), jnp.zeros((8, 128), f32), jnp.full((8, 128), -jnp.inf, f32)]
        for t in range(9):
            lanes = slice(t * 128, t * 128 + 128)
            sums = []
            for k, (a_ref, b_ref) in enumerate(((num_a_ref, num_b_ref), (den_a_ref, den_b_ref))):
                whole = jnp.concatenate(
                    [
                        a_ref[0:mid, lanes],
                        a_ref[mid : mid + 16, lanes] + b_ref[0:16, lanes],
                        b_ref[16 : mid + 16, lanes],
                    ],
                    axis=0,
                )
                if t == 8:
                    whole = whole + side_ref[2 * k]
                elif t in (0, 7):
                    edge = side_ref[2 * k + 1]
                    before = lane_iota(edge.shape) < 64
                    whole = whole + jnp.where(before == (t == 0), edge, 0.0)
                sums.append(whole)
            num, den = sums
            value = num / jnp.maximum(den, floor_value)
            product = den * value
            inner = slice(16, count - 16)
            p1_ref[0:16, lanes] = num[0:16]
            p1_ref[inner, lanes] = product[inner]
            p1_ref[count - 16 : count, lanes] = num[count - 16 : count]
            c1_ref[:, lanes] = den
            if t < 8:
                one_ref[8 : count - 24, lanes] = value[inner]
                part[0] = part[0] + jnp.sum(fold(product[inner]), 0)
                part[1] = part[1] + jnp.sum(fold(den[inner]), 0)
                part[2] = jnp.maximum(part[2], jnp.max(fold(value[inner]), 0))
        for k in range(3):
            part_ref[k] = part[k]


def first_kernel(
    whole_ref, field_ref, words_ref, cos_ref, band_ref,
    num_ref, den_ref, lower_ref, *scratch, skip,
):
    height = lower_ref.shape[0]
    copy = pltpu.make_async_copy(
        whole_ref.at[height : 2 * height, :], lower_ref, scratch[-1].at[0]
    )

    @pl.when(pl.program_id(0) == 0)
    def _():
        copy.start()

    upper_kernel(field_ref, words_ref, cos_ref, band_ref, num_ref, den_ref, *scratch[:-1], skip=skip)

    @pl.when(pl.program_id(0) == pl.num_programs(0) - 1)
    def _():
        copy.wait()


def upper_kernel(
    field_ref, words_ref, cos_ref, band_ref, num_ref, den_ref,
    product_ref, cover_ref, main_ref, edge_ref, sheet_ref,
    *, skip,
):
    step = pl.program_id(0)
    blocks = pl.num_programs(0) - 1
    height = field_ref.shape[0] // blocks
    origin = pl.multiple_of(step * height, 128)
    line = pl.multiple_of((skip + step) * height, 128)

    @pl.when(step == 0)
    def _():
        sheet_ref[:, :, 0:24, :] = jnp.zeros((2, 9, 24, 128), f32)
        sheet_ref[:, :, 24 + 2 * height :, :] = jnp.zeros(
            (2, 9, sheet_ref.shape[2] - 24 - 2 * height, 128), f32
        )

    @pl.when(step < blocks)
    def _():
        wide = words_wide(words_ref[:, pl.ds(line, height)])
        for tile in range(8):
            part = slice(tile * height, tile * height + height)
            for half in range(2):
                lanes = slice(tile * 256 + half * 128, tile * 256 + half * 128 + 128)
                mask = land_mask(wide, 2 * tile + half)
                high, low = split(
                    jnp.where(mask, field_ref[pl.ds(origin, height), lanes], 0.0)
                )
                product_ref[part, half * 128 : half * 128 + 128] = high
                product_ref[part, 256 + half * 128 : 384 + half * 128] = low
                cover_ref[part, half * 128 : half * 128 + 128] = jnp.where(mask, 1.0, 0.0).astype(
                    bf16
                )
        cos = down_rows(cos_ref[pl.ds(skip + step, 1), :], 128)
        low_half = lane_iota((height, 128)) < 64
        start = pl.multiple_of(24 + step * height, 8)
        for which, (lhs_ref, depth) in enumerate(((product_ref, 512), (cover_ref, 256))):
            across = dot(lhs_ref[...], band_ref[0:depth, :])
            main_ref[...] = across[:, 0:128]
            edge_ref[...] = across[:, 128:256]
            zero = jnp.zeros((height, 128), f32)
            for t in range(9):
                get = lambda ref, k: ref[k * height : k * height + height, :]
                main = get(main_ref, t) if t < 8 else zero
                before = get(edge_ref, t - 1) if t > 0 else zero
                after = get(edge_ref, (t + 1) % 9) if t != 7 else zero
                sheet_ref[which, t, pl.ds(start, height), :] = (
                    main + jnp.where(low_half, before, after)
                ) * cos

    def down(count):
        first = 7 + step * height
        place = pl.multiple_of(step * (height // 2), 8)
        for which, out_ref in ((0, num_ref), (1, den_ref)):
            for t in range(9):
                out_ref[pl.ds(place, count), t * 128 : t * 128 + 128] = rows_down(
                    sheet_ref, first, count, which, t
                )

    @pl.when(step < blocks)
    def _():
        down(height // 2)

    @pl.when(step == blocks)
    def _():
        down(16)


def own_level(field, words, cosines, band, part, *beside):
    height = 128
    blocks = field.shape[0] // height
    rows, cols = 2 * field.shape[0], field.shape[1]
    skip = part * blocks
    vmem = pl.BlockSpec(memory_space=pltpu.VMEM)
    half = pltpu.VMEM((blocks * height // 2 + 16, cols // 2 + 128), f32)
    if part == 0:
        kernel, given = first_kernel, [pl.BlockSpec(memory_space=pl.ANY)]
        outs = [half, half, pltpu.VMEM(field.shape, f32)]
        scratch = [pltpu.SemaphoreType.DMA((1,))]
    else:
        kernel, given = lower_kernel, [vmem] * 4
        level = pltpu.VMEM((rows // 2 + 16, cols // 2 + 128), f32)
        outs = [level, level, pltpu.VMEM((rows // 2, cols // 2), f32), pltpu.VMEM((3, 8, 128), f32)]
        scratch = [
            half,
            half,
            pltpu.VMEM((4, rows // 2 + 16, 128), f32),
            pltpu.VMEM((4, rows + 48, 128), f32),
        ]
    return pl.pallas_call(
        functools.partial(kernel, skip=skip),
        grid=(blocks + 1,),
        in_specs=given + [vmem] * 4,
        out_specs=[vmem] * len(outs),
        out_shape=outs,
        scratch_shapes=[
            pltpu.VMEM((8 * height, 512), bf16),
            pltpu.VMEM((8 * height, 256), bf16),
            pltpu.VMEM((8 * height, 128), f32),
            pltpu.VMEM((8 * height, 128), f32),
            pltpu.VMEM((2, 9, 24 + (blocks + 1) * height, 128), f32),
            *scratch,
        ],
        compiler_params=pltpu.CompilerParams(vmem_limit_bytes=vmem_limit),
        name="own_level",
    )(*beside, field, words, cosines, band)


def levels_kernel(
    place_ref, p1_ref, c1_ref, part_ref, core_ref, chip_ref, band_ref, band_halo_ref,
    head_ref, tail_ref, two_ref, three_ref, four_ref, stats_ref,
    ends_ref, p2_ref, c2_ref, p3_ref, c3_ref, tall_ref, strip_ref, value_ref,
    *, last_place,
):
    count = p1_ref.shape[0]
    rows = 2 * (count - 16)
    band = band_ref[...]
    odd = (place_ref[0] & 1) == 1
    tall_ref[:, 0:8, :] = jnp.zeros((4, 8, 128), f32)

    def pick(before, after):
        shape = before.shape
        return jnp.where(lane_iota(shape) < 64, before, after)

    strip_ref[...] = jnp.zeros(strip_ref.shape, f32)
    for side, first in ((0, 8), (1, 24)):
        of_core = odd if side == 0 else jnp.logical_not(odd)
        strip = jnp.where(of_core, core_ref[...], chip_ref[...])
        for which in range(2):
            for t in range(9):
                strip_ref[side, which, t, first : first + 16, :] = strip[
                    which * 16 : which * 16 + 16, t * 128 : t * 128 + 128
                ]

    at_first = (place_ref[0] == 0).astype(jnp.int32)
    at_last = (place_ref[0] == last_place).astype(jnp.int32)
    sums = []

    def finish(num, den, halo, own):
        value = num / jnp.maximum(den, floor_value)
        row = lax.broadcasted_iota(jnp.int32, num.shape, 0)
        inside = (row >= halo * at_first) & (row < own + halo + (1 - at_last) * 4096)
        cover = jnp.where(inside, den, 0.0)
        return value, cover * value, cover

    level_one_sums = tuple(part_ref[k] for k in range(3))
    row = lax.broadcasted_iota(jnp.int32, (16, 128), 0)
    for side in range(2):
        where = slice(0, 16) if side == 0 else slice(count - 16, count)
        own = slice(8, 16) if side == 0 else slice(0, 8)
        inside = (row >= 8 * at_first) if side == 0 else (row < 8 + (1 - at_last) * 8)
        out_ref = head_ref if side == 0 else tail_ref
        for t in range(9):
            lanes = slice(t * 128, t * 128 + 128)
            num = p1_ref[where, lanes] + rows_down(strip_ref, 7, 16, side, 0, t)
            den = c1_ref[where, lanes] + rows_down(strip_ref, 7, 16, side, 1, t)
            value = num / jnp.maximum(den, floor_value)
            cover = jnp.where(inside, den, 0.0)
            product = cover * value
            ends_ref[side, 0, :, lanes] = product
            ends_ref[side, 1, :, lanes] = cover
            if t < 8:
                out_ref[:, lanes] = value[own]
                old = level_one_sums
                level_one_sums = (
                    old[0] + product[own], old[1] + cover[own], jnp.maximum(old[2], value[own])
                )
    sums.append(level_one_sums)

    def next_level(p_ref, c_ref, tiles, in_rows, out_rows, halo, own_rows, out_ref, p_out, c_out):
        total = None
        nums = []
        dens = []
        for which, (ref, dest) in enumerate(((p_ref, nums), (c_ref, dens))):
            blocks = []

            def part(first, width):
                lanes = slice(first, first + width)
                if ref.shape[0] != count:
                    return ref[:, lanes]
                ends = [ends_ref[side, which, :, lanes] for side in range(2)]
                return jnp.concatenate([ends[0], ref[16 : count - 16, lanes], ends[1]], axis=0)

            for t in range(tiles):
                blocks.append(dot(split_pair(part(t * 256, 256)), band))
            blocks.append(dot(split_pair(part(tiles * 256, 128)), band_halo_ref[...]))
            ring_tiles = tiles + 1
            for t in range(ring_tiles):
                across = blocks[t][:, 0:128] + pick(
                    blocks[(t - 1) % ring_tiles][:, 128:256],
                    blocks[(t + 1) % ring_tiles][:, 128:256],
                )
                slot = t % 4
                tall_ref[slot, 8 : 8 + in_rows, :] = across
                tall_ref[slot, 8 + in_rows : 2 * out_rows + 16, :] = jnp.zeros(
                    (2 * out_rows + 8 - in_rows, 128), f32
                )
                dest.append(rows_down(tall_ref, 7, out_rows, slot))
        for t in range(tiles + 1):
            value, product, cover = finish(nums[t], dens[t], halo, own_rows)
            if p_out is not None:
                p_out[:, t * 128 : t * 128 + 128] = product
                c_out[:, t * 128 : t * 128 + 128] = cover
            if t < tiles:
                own = slice(halo, halo + own_rows)
                value_ref[0, 0:out_rows, :] = value
                value_ref[1, 0:out_rows, :] = product
                value_ref[2, 0:out_rows, :] = cover
                v, p, c = (value_ref[k, own, :] for k in range(3))
                out_ref[:, t * 128 : t * 128 + 128] = v
                new = (jnp.sum(fold(p), 0), jnp.sum(fold(c), 0), jnp.max(fold(v), 0))
                total = (
                    new
                    if total is None
                    else (total[0] + new[0], total[1] + new[1], jnp.maximum(total[2], new[2]))
                )
        sums.append(total)

    next_level(p1_ref, c1_ref, 4, 272, 136, 4, 128, two_ref, p2_ref, c2_ref)
    next_level(p2_ref, c2_ref, 2, 136, 72, 2, 64, three_ref, p3_ref, c3_ref)
    next_level(p3_ref, c3_ref, 1, 72, 40, 1, 32, four_ref, None, None)

    lane = lane_iota((1, 128))
    row = jnp.zeros((1, 128), f32)
    for level in range(4):
        for kind in range(3):
            part = sums[level][kind]
            one = (jnp.max if kind == 2 else jnp.sum)(part, axis=0, keepdims=True)
            one = (jnp.max if kind == 2 else jnp.sum)(one, axis=1, keepdims=True)
            row = jnp.where(lane == kind * 4 + level, one, row)
    stats_ref[...] = jnp.broadcast_to(row, stats_ref.shape)


def all_levels(place, last_place, chips, level_one, by_core, by_chip, tables, rows, cols):
    vmem = pl.BlockSpec(memory_space=pltpu.VMEM)
    shapes = [(8, cols // 2)] * 2 + [(rows >> k, cols >> k) for k in (2, 3, 4)]
    outs = [pltpu.VMEM(shape, f32) for shape in shapes]
    return pl.pallas_call(
        functools.partial(levels_kernel, last_place=last_place),
        in_specs=[pl.BlockSpec(memory_space=pltpu.SMEM)] + [vmem] * 7,
        out_specs=[vmem] * 6,
        out_shape=outs + [pltpu.VMEM((chips, 128), f32)],
        scratch_shapes=[
            pltpu.VMEM((2, 2, 16, cols // 2 + 128), f32),
            pltpu.VMEM((136, cols // 4 + 128), f32),
            pltpu.VMEM((136, cols // 4 + 128), f32),
            pltpu.VMEM((72, cols // 8 + 128), f32),
            pltpu.VMEM((72, cols // 8 + 128), f32),
            pltpu.VMEM((4, rows + 48, 128), f32),
            pltpu.VMEM((2, 2, 9, 48, 128), f32),
            pltpu.VMEM((3, 136, 128), f32),
        ],
        compiler_params=pltpu.CompilerParams(vmem_limit_bytes=vmem_limit),
        name="all_levels",
    )(place, *level_one, by_core, by_chip, *tables)


def emit_kernel(
    after_ref, one_ref, head_ref, tail_ref, two_ref, three_ref, four_ref,
    one_out, two_out, three_out, four_out, sems,
):
    del after_ref
    count = one_ref.shape[0]
    pairs = (
        (one_ref.at[8 : count - 8, :], one_out.at[8 : count - 8, :]),
        (head_ref, one_out.at[0:8, :]),
        (tail_ref, one_out.at[count - 8 : count, :]),
        (two_ref, two_out),
        (three_ref, three_out),
        (four_ref, four_out),
    )
    copies = [pltpu.make_async_copy(*pair, sems.at[k]) for k, pair in enumerate(pairs)]
    for copy in copies:
        copy.start()
    for copy in copies:
        copy.wait()


def emit(after, one, head, tail, *rest):
    levels = (one, *rest)
    return pl.pallas_call(
        emit_kernel,
        in_specs=[pl.BlockSpec(memory_space=pltpu.VMEM)] * 7,
        out_specs=[pl.BlockSpec(memory_space=pl.ANY)] * 4,
        out_shape=[jax.ShapeDtypeStruct(level.shape, f32) for level in levels],
        scratch_shapes=[pltpu.SemaphoreType.DMA((6,))],
        compiler_params=pltpu.CompilerParams(vmem_limit_bytes=vmem_limit),
        name="emit",
    )(after, *[on_chip(level) for level in (one, head, tail, *rest)])


def per_device(surface_field, land_words):
    rows, cols = surface_field.shape
    row_devices = lax.axis_size(ROWS)
    col_devices = lax.axis_size(COLS)
    total_rows = rows * row_devices
    position = lax.axis_index(ROWS)

    band = jnp.asarray(band_main(), bf16)
    mixed = jnp.asarray(
        np.concatenate([band_halo(16, 0, 128), band_halo(16, 16, 112)], axis=1), bf16
    )

    place = jnp.reshape(position, (1,))
    words = land_words.T

    east = [(i, (i + 1) % col_devices) for i in range(col_devices)]
    west = [(target, source) for source, target in east]

    to_left, to_right, near, near_words, cosines = columns_strips(
        place, in_hbm(surface_field), in_hbm(words), total_rows
    )
    near, near_words, cosines = on_chip(near), on_chip(near_words), on_chip(cosines)
    from_right = lax.ppermute(to_left, COLS, west)
    from_left = lax.ppermute(to_right, COLS, east)
    twice = jnp.asarray(np.tile(band_main(), (2, 1)), bf16)
    ring_twice = jnp.asarray(np.tile(band_halo(64, 0, 128), (2, 1)), bf16)
    mixed_twice = jnp.concatenate([mixed, mixed], axis=0)
    *upper, lower_near = own_level(near, near_words, cosines, twice, 0, in_hbm(surface_field))
    lower_near = on_chip(lower_near)
    to_core, to_chip, halo = rows_strips(
        place, on_chip(upper[0]), near, lower_near, near_words, on_chip(from_right), on_chip(from_left),
        cosines, (band, mixed),
    )
    by_chip = lax.ppermute(to_chip, ROWS, [(i, ((i - 1) ^ 1) + 1) for i in range(1, row_devices - 1)])
    by_core = lax.ppermute(to_core, ROWS, [(i, i ^ 1) for i in range(row_devices)])
    p1, c1, one, part = own_level(
        lower_near, near_words, cosines, twice, 1,
        on_chip(halo), mixed_twice, *[on_chip(x) for x in upper],
    )
    chips = lax.axis_size(CHIPS)
    *levels, stats = all_levels(
        place, row_devices - 1, chips, [on_chip(x) for x in (p1, c1, part)],
        on_chip(by_core), on_chip(by_chip), (twice, ring_twice), rows, cols,
    )

    is_sum = jnp.arange(128) < 8
    every = lax.all_to_all(stats, CHIPS, 0, 0, tiled=True)
    stats = jnp.where(is_sum, jnp.sum(every, axis=0), jnp.max(every, axis=0))
    other = lax.ppermute(stats, CORE, [(0, 1), (1, 0)])
    one, two, three, four = emit(on_chip(stats), one, *levels)
    sums = stats[0:8] + other[0:8]
    maxima = jnp.maximum(stats[8:12], other[8:12])
    means = sums[0:4] / (sums[4:8] + mean_eps)
    return (one, two, three, four, means, maxima)


def solution(mesh):
    finer = Mesh(
        mesh.devices.reshape(2, 4, 2, 2, 4), ("rows_0", "rows_1", "rows_2", "cols_0", "cols_1")
    )
    in_specs = (P(ROWS, COLS), P(ROWS, COLS))
    out_specs = (P(ROWS, COLS), P(ROWS, COLS), P(ROWS, COLS), P(ROWS, COLS), P(), P())
    return jax.shard_map(
        per_device, mesh=finer, in_specs=in_specs, out_specs=out_specs, check_vma=False
    )
```
